256 devices in a mesh: inter: 32 (over y, z_hi, x), intra: 8 (over z_lo, core).
Axes of the slice: x: 4, y: 4, z: 8 (z_hi: 2, z_lo: 4; z = z_hi * 4 + z_lo), core: 2. Of those that a mesh axis runs over, the one named last changes fastest.
Arguments:
- tokens: bfloat16 [4096, 4096], P('inter', 'intra'), may hold values from -6 to 6
- gate_codes: bfloat16 [7168, 4096], P(('intra', 'inter')), may hold values from -127 to 127
- gate_scales: float32 [7168, 16], P(('intra', 'inter')), may hold values from 0.0001 to 0.0005
- up_codes: bfloat16 [7168, 4096], P(('intra', 'inter')), may hold values from -127 to 127
- up_scales: float32 [7168, 16], P(('intra', 'inter')), may hold values from 0.0001 to 0.0005
- cotangent: bfloat16 [4096, 7168], P('inter', 'intra'), may hold values from -6 to 6
Outputs:
- hidden: bfloat16 [4096, 7168], P('inter', 'intra')
- token_grad: bfloat16 [4096, 4096], P('inter', 'intra')
- gate_grad: float32 [7168, 4096], P(('intra', 'inter'))
- up_grad: float32 [7168, 4096], P(('intra', 'inter'))
The draws below stay inside these ranges and needn't reach their ends.
All inputs are finite; a program needn't handle non-finite values.
Results may differ from the reference program's by a relative error of at most 0.02.
Values may be sent and summed in bfloat16 or wider, within the bound.
No kernel may reach another device: no remote copies, remote signals or barrier semaphores. Data moves between devices by JAX's collectives and lax.ppermute only.
A program may use at most 192 MiB of HBM per device.

```python
import math
import jax
import jax.numpy as jnp
from jax import lax

D = 4096
FF = 7168
BLOCK = 256
TOK_DEV = 128
TOKENS = 4096
N_INTER = 32
N_INTRA = 8


def draw_gate_codes(key, part):
    values = jax.random.randint(jax.random.fold_in(key, 11), (FF, D), -127, 128)
    return values.astype(jnp.float32).astype(jnp.bfloat16)


def draw_up_codes(key, part):
    values = jax.random.randint(jax.random.fold_in(key, 23), (FF, D), -127, 128)
    return values.astype(jnp.float32).astype(jnp.bfloat16)


def levels(stream_key, extent, pieces, low, high):
    factor_of, own = 1.0, jax.random.fold_in(stream_key, 6)
    for position, parts in pieces:
        steps = jnp.exp(jax.random.uniform(jax.random.fold_in(own, position), (parts,), jnp.float32, low / len(pieces), high / len(pieces)))
        factor_of = factor_of * jnp.repeat(steps, extent[position] // parts).reshape([-1 if axis == position else 1 for axis in range(len(extent))])
    return factor_of


def bell_draw(stream_key, shape, scale, reach, cuts=(), kind=jnp.bfloat16):
    level = levels(stream_key, shape, cuts, -0.22, 0.18) if cuts else 1.0
    entries = jax.random.normal(stream_key, shape, jnp.float32) * scale * level
    return jnp.minimum(jnp.maximum(entries, -reach), reach).astype(kind)


def setup_inputs(seed: int = 0) -> dict:
    seeds = jax.random.split(jax.random.key(seed), 7)
    tokens = bell_draw(seeds[0], (TOKENS, D), 1.0, 6.0, ((0, 32), (1, 8)))
    gate_codes = draw_gate_codes(jax.random.fold_in(seeds[6], 71), 0)
    gate_scales = jnp.clip(jnp.exp(math.log(0.0005) - 1.609438 * jax.random.uniform(seeds[2], (FF, D // BLOCK), jnp.float32) ** levels(seeds[2], (FF, D // BLOCK), ((0, 256),), -0.2, 0.2)), 0.0001, 0.0005)
    up_codes = draw_up_codes(jax.random.fold_in(seeds[6], 71), 0)
    up_scales = jnp.clip(jnp.exp(math.log(0.0005) - 1.609438 * jax.random.uniform(seeds[4], (FF, D // BLOCK), jnp.float32) ** levels(seeds[4], (FF, D // BLOCK), ((0, 256),), -0.2, 0.2)), 0.0001, 0.0005)
    cotangent = bell_draw(seeds[5], (TOKENS, FF), 1.0, 6.0, ((0, 32), (1, 8)))
    return {"tokens": tokens, "gate_codes": gate_codes, "gate_scales": gate_scales, "up_codes": up_codes, "up_scales": up_scales, "cotangent": cotangent}


def dequantize(codes, scales):
    rows, width = codes.shape
    blocks = scales.shape[1]
    values = codes.astype(jnp.float32).reshape(rows, blocks, width // blocks) * scales[:, :, None]
    return values.reshape(rows, width).astype(jnp.bfloat16)


def to_wire(value):
    rounded = value.astype(jnp.bfloat16)
    rounded = lax.optimization_barrier(rounded)
    return rounded.astype(jnp.float32)


def reference(tokens, gate_codes, gate_scales, up_codes, up_scales, cotangent):
    w_gate = dequantize(gate_codes, gate_scales)
    w_up = dequantize(up_codes, up_scales)
    gate = jnp.dot(tokens, w_gate.T, preferred_element_type=jnp.float32)
    up = jnp.dot(tokens, w_up.T, preferred_element_type=jnp.float32)
    sig = jax.nn.sigmoid(gate)
    act = gate * sig
    hidden = (act * up).astype(jnp.bfloat16)
    back = cotangent.astype(jnp.float32)
    d_up = (back * act).astype(jnp.bfloat16)
    d_gate = (back * up * sig * (1.0 + gate * (1.0 - sig))).astype(jnp.bfloat16)
    width = FF // N_INTRA
    total = jnp.zeros((TOKENS, D), jnp.float32)
    for block in range(N_INTRA):
        lower = block * width
        part = jnp.dot(d_gate[:, lower:lower + width], w_gate[lower:lower + width], preferred_element_type=jnp.float32)
        part = part + jnp.dot(d_up[:, lower:lower + width], w_up[lower:lower + width], preferred_element_type=jnp.float32)
        total = total + to_wire(part)
    token_grad = total.astype(jnp.bfloat16)
    grouped_tokens = tokens.reshape(N_INTER, TOK_DEV, D)
    grouped_gate = d_gate.reshape(N_INTER, TOK_DEV, FF)
    grouped_up = d_up.reshape(N_INTER, TOK_DEV, FF)

    def accumulate(carry, group):
        rows, dgs, dus = group
        acc_gate, acc_up = carry
        term_gate = jnp.dot(dgs.T, rows, preferred_element_type=jnp.float32)
        term_up = jnp.dot(dus.T, rows, preferred_element_type=jnp.float32)
        return (acc_gate + to_wire(term_gate), acc_up + to_wire(term_up)), None

    start = (jnp.zeros((FF, D), jnp.float32), jnp.zeros((FF, D), jnp.float32))
    (sum_gate, sum_up), _ = lax.scan(accumulate, start, (grouped_tokens, grouped_gate, grouped_up))
    gate_grad = sum_gate / N_INTER
    up_grad = sum_up / N_INTER
    return hidden, token_grad, gate_grad, up_grad
```

```python
import functools
import jax
import jax.numpy as jnp
from jax import lax
from jax.experimental import pallas as pl
from jax.experimental.pallas import tpu as pltpu
from jax.sharding import PartitionSpec as P


D = 4096
TOK = 128
SLICE = 512
ROWS = 28
BLOCK = 256
NY, NZH, NX, NZL, NC = 4, 2, 4, 4, 2
NZ = NZH * NZL
GROUPS = NY * NZH * NX
REL = (0, -1, 1, 2)
HALF_A, HALF_B = 16, 12
SHARD_A, SHARD_B = 2 * HALF_A, 2 * HALF_B
WIDE_A, WIDE_B = 16 * SHARD_A, 16 * SHARD_B
WIDE = WIDE_A + WIDE_B
F32, BF16 = jnp.float32, jnp.bfloat16
VMEM_LIMIT = 56 * 1024 * 1024


def shift(value, dx=0, dy=0, dz=0, dc=0):
    pairs = []
    for y in range(NY):
        for zh in range(NZH):
            for x in range(NX):
                for zl in range(NZL):
                    for c in range(NC):
                        z = (zh * NZL + zl + dz) % NZ
                        source = (((y * NZH + zh) * NX + x) * NZL + zl) * NC + c
                        target = (
                            (((y + dy) % NY * NZH + z // NZL) * NX + (x + dx) % NX) * NZL + z % NZL
                        ) * NC + (c + dc) % NC
                        pairs.append((source, target))
    return lax.ppermute(value, ("inter", "intra"), pairs)


def call(kernel, outs, name, **kw):
    return pl.pallas_call(
        kernel,
        out_shape=outs,
        name=name,
        compiler_params=pltpu.CompilerParams(vmem_limit_bytes=VMEM_LIMIT),
        **kw,
    )


def shape(rows, cols, kind=BF16):
    return jax.ShapeDtypeStruct((rows, cols), kind)


SMEM = pl.BlockSpec(memory_space=pltpu.SMEM)
VMEM = pl.BlockSpec(memory_space=pltpu.VMEM)


def dequant_kernel(gc, gs, uc, us, a, b):
    for n in range(D // BLOCK):
        cols = slice(n * BLOCK, (n + 1) * BLOCK)
        g = gc[:, cols].astype(F32) * gs[:, n : n + 1]
        u = uc[:, cols].astype(F32) * us[:, n : n + 1]
        a[:, cols] = jnp.concatenate([g[:HALF_A], u[:HALF_A]], axis=0).astype(BF16)
        b[:, cols] = jnp.concatenate([g[HALF_A:], u[HALF_A:]], axis=0).astype(BF16)


def place_kernel(slots, *refs):
    pieces, out = refs[:-1], refs[-1]
    for n, piece in enumerate(pieces):
        out[slots[n]] = piece[...]


def join_kernel(core, own, other, out):
    c = core[0]
    for t in range(2):
        for zl in range(NZL):
            rows = slice(t * TOK, (t + 1) * TOK)
            mine = pl.multiple_of((zl * NC + c) * SLICE, SLICE)
            theirs = pl.multiple_of((zl * NC + 1 - c) * SLICE, SLICE)
            out[rows, pl.ds(mine, SLICE)] = own[t * NZL + zl]
            out[rows, pl.ds(theirs, SLICE)] = other[t * NZL + zl]


def gating(gu, cot, shard, half):
    width = gu.shape[1]
    gate = gu
    up = pltpu.roll(gu, width - half, 1)
    sig = jax.nn.sigmoid(gate)
    act = gate * sig
    d_up = cot * act
    d_gate = cot * up * sig * (1.0 + gate * (1.0 - sig))
    first = lax.broadcasted_iota(jnp.int32, gu.shape, 1) % shard < half
    hidden = jnp.where(first, act * up, 0.0)
    both = jnp.where(first, d_gate, pltpu.roll(d_up, half, 1))
    return hidden.astype(BF16), both.astype(BF16)


def forward_kernel(x, cot, *refs):
    wa, wb = refs[:5], refs[5:10]
    hidden, dd_a, dd_b, acc_a, acc_b = refs[10:]
    step = pl.program_id(0)

    @pl.when(step == 0)
    def _():
        acc_a[...] = jnp.zeros_like(acc_a)
        acc_b[...] = jnp.zeros_like(acc_b)

    dims = (((1,), (1,)), ((), ()))
    w = jnp.concatenate([r[...] for r in wa], axis=0)
    acc_a[...] += lax.dot_general(x[...], w, dims, preferred_element_type=F32)
    w = jnp.concatenate([r[...] for r in wb], axis=0)
    acc_b[...] += lax.dot_general(x[...], w, dims, preferred_element_type=F32)

    @pl.when(step == pl.num_programs(0) - 1)
    def _():
        h, d = gating(acc_a[...], cot[:, :WIDE_A].astype(F32), SHARD_A, HALF_A)
        hidden[:, :WIDE_A] = h
        dd_a[...] = d
        h, d = gating(acc_b[...], cot[:, WIDE_A:].astype(F32), SHARD_B, HALF_B)
        hidden[:, WIDE_A:] = h
        dd_b[...] = d


def weight_grad_kernel(dd, x, own, left, right, far_lo, far_hi):
    g = lax.dot_general(dd[...], x[...], (((0,), (0,)), ((), ())), preferred_element_type=F32)
    lower = 0
    for out in (own, left, right, far_lo, far_hi):
        n = out.shape[0]
        out[...] = g[lower : lower + n].astype(BF16)
        lower += n


def token_grad_kernel(core, dd_a, dd_b, *refs):
    wa, wb = refs[:5], refs[5:10]
    own, other = refs[10:]
    dims = (((1,), (0,)), ((), ()))
    dd = jnp.concatenate([dd_a[...], dd_b[...]], axis=1)
    mine = core[0]
    for c in range(NC):
        cols = slice(c * SLICE, (c + 1) * SLICE)
        w = jnp.concatenate([r[:, cols] for r in wa + wb], axis=0)
        p = lax.dot_general(dd, w, dims, preferred_element_type=F32).astype(BF16)
        p = p.reshape(2, 1, TOK, SLICE)

        @pl.when(mine == c)
        def _():
            own[...] = p

        @pl.when(mine != c)
        def _():
            other[...] = p


def pair_sum_kernel(slots, own, other, *outs):
    for n, out in enumerate(outs):
        s = slots[n]
        out[...] = (own[s].astype(F32) + other[s].astype(F32)).astype(BF16)


def total_kernel(*refs):
    total = refs[0][...].astype(F32)
    for r in refs[1:-1]:
        total = total + r[...].astype(F32)
    refs[-1][...] = total.astype(BF16)


def relay_kernel(left, right, from_right, from_left, left_out, right_out):
    n = from_right.shape[0]
    left_out[...] = (left[...].astype(F32) + from_right[...].astype(F32)).astype(BF16)
    right_out[...] = (right[...].astype(F32) + from_left[...].astype(F32)).astype(BF16)


def stage_kernel(own, r_lo, r_hi, l_lo, l_hi, *outs):
    half = own.shape[0] // 2
    rows = own.shape[0] // 4
    lo = own[:half].astype(F32) + r_lo[...].astype(F32) + l_lo[...].astype(F32)
    hi = own[half:].astype(F32) + r_hi[...].astype(F32) + l_hi[...].astype(F32)
    outs[0][...] = lo[:rows].astype(BF16)
    outs[1][...] = lo[rows:].astype(BF16)
    outs[2][...] = hi[:rows].astype(BF16)
    outs[3][...] = hi[rows:].astype(BF16)


def finish_kernel(*refs):
    a, b, gate, up = refs[:4], refs[4:8], refs[8], refs[9]
    ta = sum(r[...].astype(F32) for r in a) * (1.0 / GROUPS)
    tb = sum(r[...].astype(F32) for r in b) * (1.0 / GROUPS)
    gate[...] = jnp.concatenate([ta[:HALF_A], tb[:HALF_B]], axis=0)
    up[...] = jnp.concatenate([ta[HALF_A:], tb[HALF_B:]], axis=0)


def gather_plane(shard, first, second):
    near = [shard] + [shift(shard, **{first: -r}) for r in REL[1:]]
    own = jnp.concatenate(near, axis=0)
    n = own.shape[0] // 2
    left = shift(own, **{second: 1})
    right = shift(own, **{second: -1})
    far_lo = shift(left[:n], **{second: 1})
    far_hi = shift(right[n:], **{second: -1})
    return own, left, right, far_lo, far_hi


def reduce_plane(parts, first, second):
    own, left, right, far_lo, far_hi = parts
    n = far_lo.shape[0]
    from_right = shift(far_lo, **{second: -1})
    from_left = shift(far_hi, **{second: 1})
    r_hi = shift(left[n:], **{second: -1})
    l_lo = shift(right[:n], **{second: 1})
    left_lo, right_hi = call(
        relay_kernel, (shape(n, D), shape(n, D)), "relay"
    )(left[:n], right[n:], from_right, from_left)
    r_lo = shift(left_lo, **{second: -1})
    l_hi = shift(right_hi, **{second: 1})
    rows = n // 2
    pieces = call(stage_kernel, tuple(shape(rows, D) for _ in REL), "stage")(
        own, r_lo, r_hi, l_lo, l_hi
    )
    return [pieces[0]] + [shift(p, **{first: r}) for p, r in zip(pieces[1:], REL[1:])]


def per_device(tokens, gate_codes, gate_scales, up_codes, up_scales, cotangent):
    inter, intra = lax.axis_index("inter"), lax.axis_index("intra")
    y, zh, x = inter // (NZH * NX), inter // NX % NZH, inter % NX
    zl, core = intra // NC, intra % NC
    z = zh * NZL + zl
    core_id = core.reshape(1).astype(jnp.int32)
    steps = (0, 1, -1, 2, -2, 3, -3, 4)

    def slot(step):
        there = (z + step) % NZ
        return jnp.where(there // NZL == zh, 0, NZL) + there % NZL

    slots_in = jnp.stack([slot(-s) for s in steps]).astype(jnp.int32)
    slots_out = jnp.stack([slot(s) for s in steps]).astype(jnp.int32)

    shard_a, shard_b = call(dequant_kernel, (shape(SHARD_A, D), shape(SHARD_B, D)), "dequant")(
        gate_codes, gate_scales, up_codes, up_scales
    )
    wa = gather_plane(shard_a, "dx", "dy")
    wb = gather_plane(shard_b, "dy", "dx")

    cube = jax.ShapeDtypeStruct((NZ, TOK, SLICE), BF16)
    pieces = [tokens] + [shift(tokens, dz=s) for s in steps[1:]]
    mine = call(
        place_kernel, cube, "place", in_specs=[SMEM] + [VMEM] * NZ, out_specs=VMEM
    )(slots_in, *pieces)
    theirs = shift(mine, dc=1)
    whole = call(
        join_kernel, shape(2 * TOK, D), "join", in_specs=[SMEM, VMEM, VMEM], out_specs=VMEM
    )(core_id, mine, theirs)

    rel = jnp.array(REL, jnp.int32)
    shards = jnp.arange(16, dtype=jnp.int32)
    ya, xa = (y + rel[shards // 4]) % NY, (x + rel[shards % 4]) % NX
    yb, xb = (y + rel[shards % 4]) % NY, (x + rel[shards // 4]) % NX

    def origin(half):
        base_a = ((ya * NZH + half) * NX + xa) * ROWS
        base_b = ((yb * NZH + half) * NX + xb) * ROWS + HALF_A
        ra, rb = jnp.arange(SHARD_A), jnp.arange(SHARD_B)
        oa = jnp.where(ra < HALF_A, base_a[:, None] + ra, -1).reshape(WIDE_A)
        ob = jnp.where(rb < HALF_B, base_b[:, None] + rb, -1).reshape(WIDE_B)
        return jnp.concatenate([oa, ob])

    columns = jnp.concatenate([origin(zh), origin(1 - zh)])
    pick = (jnp.arange(GROUPS * ROWS)[:, None] == columns[None, :]).astype(BF16)
    spread = jnp.dot(cotangent, pick, preferred_element_type=F32).astype(BF16)
    cot = jnp.concatenate([spread[:, :WIDE], shift(spread[:, WIDE:], dz=4)], axis=0)

    chunk = 1024
    grid = (D // chunk,)

    def cols(rows, width=chunk):
        return pl.BlockSpec((rows, width), lambda j: (0, j))

    def full(*dims):
        return pl.BlockSpec(dims, lambda j: (0,) * len(dims))

    w_specs = [cols(w.shape[0]) for w in wa + wb]
    hidden_wide, dd_a, dd_b = call(
        forward_kernel,
        (shape(2 * TOK, WIDE), shape(2 * TOK, WIDE_A), shape(2 * TOK, WIDE_B)),
        "forward",
        grid=grid,
        in_specs=[cols(2 * TOK), full(2 * TOK, WIDE)] + w_specs,
        out_specs=(full(2 * TOK, WIDE), full(2 * TOK, WIDE_A), full(2 * TOK, WIDE_B)),
        scratch_shapes=[pltpu.VMEM((2 * TOK, WIDE_A), F32), pltpu.VMEM((2 * TOK, WIDE_B), F32)],
    )(whole, cot, *wa, *wb)

    def weight_grad(dd, parts, name):
        return call(
            weight_grad_kernel,
            tuple(shape(p.shape[0], D) for p in parts),
            name,
            grid=grid,
            in_specs=[full(*dd.shape), cols(2 * TOK)],
            out_specs=tuple(cols(p.shape[0]) for p in parts),
        )(dd, whole)

    sums_a = reduce_plane(weight_grad(dd_a, wa, "grad_a"), "dx", "dy")
    sums_b = reduce_plane(weight_grad(dd_b, wb, "grad_b"), "dy", "dx")
    gate_grad, up_grad = call(
        finish_kernel, (shape(ROWS, D, F32), shape(ROWS, D, F32)), "finish"
    )(*sums_a, *sums_b)

    quad = pl.BlockSpec((2, 1, TOK, SLICE), lambda j: (0, j, 0, 0))
    quad_shape = jax.ShapeDtypeStruct((2, NZL, TOK, SLICE), BF16)
    own_tg, other_tg = call(
        token_grad_kernel,
        (quad_shape, quad_shape),
        "token_grad",
        grid=(NZL,),
        in_specs=[SMEM, full(2 * TOK, WIDE_A), full(2 * TOK, WIDE_B)]
        + [cols(w.shape[0], NC * SLICE) for w in wa + wb],
        out_specs=(quad, quad),
    )(core_id, dd_a, dd_b, *wa, *wb)
    received = shift(other_tg, dc=1)
    blocks = call(
        pair_sum_kernel,
        tuple(shape(TOK, SLICE) for _ in steps),
        "pair_sum",
        in_specs=[SMEM, VMEM, VMEM],
        out_specs=tuple(VMEM for _ in steps),
    )(slots_out, own_tg.reshape(NZ, TOK, SLICE), received.reshape(NZ, TOK, SLICE))
    arrived = [blocks[0]] + [shift(b, dz=s) for b, s in zip(blocks[1:], steps[1:])]
    token_grad = call(total_kernel, shape(TOK, SLICE), "total")(*arrived)

    back = jnp.concatenate([hidden_wide[:TOK], shift(hidden_wide[TOK:], dz=4)], axis=1)
    hidden = lax.dot_general(
        back, pick, (((1,), (1,)), ((), ())), preferred_element_type=F32
    ).astype(BF16)
    return hidden, token_grad, gate_grad, up_grad


def solution(mesh):
    return jax.shard_map(
        per_device,
        mesh=mesh,
        in_specs=(
            P("inter", "intra"),
            P(("intra", "inter"), None),
            P(("intra", "inter"), None),
            P(("intra", "inter"), None),
            P(("intra", "inter"), None),
            P("inter", "intra"),
        ),
        out_specs=(
            P("inter", "intra"),
            P("inter", "intra"),
            P(("intra", "inter"), None),
            P(("intra", "inter"), None),
        ),
        check_vma=False,
    )
```

```python
import functools
import jax
import jax.numpy as jnp
from jax import lax
from jax.experimental import pallas as pl
from jax.experimental.pallas import tpu as pltpu
from jax.sharding import Mesh, PartitionSpec as P


D = 4096
TOK = 128
SLICE = 512
ROWS = 28
BLOCK = 256
NY, NZH, NX, NZL, NC = 4, 2, 4, 4, 2
NZ = NZH * NZL
GROUPS = NY * NZH * NX
REL = (0, -1, 1, 2)
HALF_A, HALF_B = 16, 12
SHARD_A, SHARD_B = 2 * HALF_A, 2 * HALF_B
WIDE_A, WIDE_B = 16 * SHARD_A, 16 * SHARD_B
WIDE = WIDE_A + WIDE_B
F32, BF16 = jnp.float32, jnp.bfloat16


AXES = ("y", "zh", "x", "zl", "core")


def shift(value, dx=0, dy=0, dz=0, dc=0):
    pairs = []
    for y in range(NY):
        for zh in range(NZH):
            for x in range(NX):
                for zl in range(NZL):
                    for c in range(NC):
                        z = (zh * NZL + zl + dz) % NZ
                        source = (((y * NZH + zh) * NX + x) * NZL + zl) * NC + c
                        target = (
                            (((y + dy) % NY * NZH + z // NZL) * NX + (x + dx) % NX) * NZL + z % NZL
                        ) * NC + (c + dc) % NC
                        pairs.append((source, target))
    return lax.ppermute(value, AXES, pairs)


def exchange_z(value):
    return lax.all_to_all(value, ("zh", "zl"), 0, 0, tiled=True)


def call(kernel, outs, megabytes=16, **kw):
    return pl.pallas_call(
        kernel,
        out_shape=outs,
        compiler_params=pltpu.CompilerParams(vmem_limit_bytes=megabytes * 1024 * 1024),
        **kw,
    )


def shape(rows, cols, kind=BF16):
    return jax.ShapeDtypeStruct((rows, cols), kind)


VMEM = pl.BlockSpec(memory_space=pltpu.VMEM)


def dequant_kernel(gc, gs, uc, us, a, b):
    scales_g, scales_u = gs[...].T, us[...].T
    for n in range(D // BLOCK):
        cols = slice(n * BLOCK, (n + 1) * BLOCK)
        g = gc[:, cols].astype(F32) * scales_g[:, n : n + 1]
        u = uc[:, cols].astype(F32) * scales_u[:, n : n + 1]
        a[:, cols] = jnp.concatenate([g[:HALF_A], u[:HALF_A]], axis=0).astype(BF16)
        b[:, cols] = jnp.concatenate([g[HALF_A:], u[HALF_A:]], axis=0).astype(BF16)


def rel_of(n):
    return jnp.where(n == 1, 3, jnp.where(n == 2, 1, jnp.where(n == 3, 2, 0)))


def spread_kernel(cot, mine, partner, pick):
    y, zh, x = lax.axis_index("y"), lax.axis_index("zh"), lax.axis_index("x")
    for flip, out in ((0, mine), (1, partner)):
        half = jnp.bitwise_xor(zh, flip)
        col = lax.broadcasted_iota(jnp.int32, (1, WIDE_A), 1)
        s, r = col // SHARD_A, col % SHARD_A
        yy, xx = (y + rel_of(s // 4)) % NY, (x + rel_of(s % 4)) % NX
        a = jnp.where(r < HALF_A, ((yy * NZH + half) * NX + xx) * ROWS + r, -1)
        col = lax.broadcasted_iota(jnp.int32, (1, WIDE_B), 1)
        s, r = col // SHARD_B, col % SHARD_B
        yy, xx = (y + rel_of(s % 4)) % NY, (x + rel_of(s // 4)) % NX
        b = jnp.where(r < HALF_B, ((yy * NZH + half) * NX + xx) * ROWS + HALF_A + r, -1)
        origin = jnp.concatenate([a, b], axis=1)
        rows = lax.broadcasted_iota(jnp.int32, (GROUPS * ROWS, WIDE), 0)
        hot = (rows == origin).astype(F32).astype(BF16)
        pick[:, flip * WIDE : (flip + 1) * WIDE] = hot
        out[...] = jnp.dot(cot[...], hot, preferred_element_type=F32).astype(BF16)


def collect_kernel(mine, partner, pick, out):
    both = jnp.concatenate([mine[...], partner[...]], axis=1)
    dims = (((1,), (1,)), ((), ()))
    out[...] = lax.dot_general(both, pick[...], dims, preferred_element_type=F32).astype(BF16)


def join_kernel(own, other, out):
    c, zh = lax.axis_index("core"), lax.axis_index("zh")
    for t in range(2):
        first = jnp.bitwise_xor(zh, t) * NZL
        for zl in range(NZL):
            rows = slice(t * TOK, (t + 1) * TOK)
            mine = pl.multiple_of((zl * NC + c) * SLICE, SLICE)
            theirs = pl.multiple_of((zl * NC + 1 - c) * SLICE, SLICE)
            out[rows, pl.ds(mine, SLICE)] = own[first + zl]
            out[rows, pl.ds(theirs, SLICE)] = other[first + zl]


def gating(gu, cot, shard, half):
    width = gu.shape[1]
    gate = gu
    up = pltpu.roll(gu, width - half, 1)
    sig = jax.nn.sigmoid(gate)
    act = gate * sig
    d_up = cot * act
    d_gate = cot * up * sig * (1.0 + gate * (1.0 - sig))
    first = lax.broadcasted_iota(jnp.int32, gu.shape, 1) % shard < half
    hidden = jnp.where(first, act * up, 0.0)
    both = jnp.where(first, d_gate, pltpu.roll(d_up, half, 1))
    return hidden.astype(BF16), both.astype(BF16)


def forward_kernel(shard, half, lower, x, cot_mine, cot_partner, *refs):
    w_refs = refs[:8]
    hidden_mine, hidden_partner, dd, acc = refs[8:]
    step = pl.program_id(0)

    @pl.when(step == 0)
    def _():
        acc[...] = jnp.zeros_like(acc)

    dims = (((1,), (1,)), ((), ()))
    w = jnp.concatenate([r[...] for r in w_refs], axis=0)
    acc[...] += lax.dot_general(x[...], w, dims, preferred_element_type=F32)

    @pl.when(step == pl.num_programs(0) - 1)
    def _():
        width = acc.shape[1]
        for rows, cot, hidden in (
            (slice(0, TOK), cot_mine, hidden_mine),
            (slice(TOK, 2 * TOK), cot_partner, hidden_partner),
        ):
            back = cot[:, lower : lower + width].astype(F32)
            hidden[...], dd[rows, :] = gating(acc[rows, :], back, shard, half)


def weight_grad_kernel(dd, x, *outs):
    g = lax.dot_general(dd[...], x[...], (((0,), (0,)), ((), ())), preferred_element_type=F32)
    n = outs[0].shape[0]
    for i, out in enumerate(outs):
        out[...] = g[i * n : (i + 1) * n].astype(BF16)


def token_grad_kernel(dd_a, dd_b, *refs):
    w_refs = refs[:16]
    own, other = refs[16:]
    mine = lax.axis_index("core")
    dims = (((1,), (0,)), ((), ()))
    dd = jnp.concatenate([dd_a[...], dd_b[...]], axis=1)
    for c in range(NC):
        cols = slice(c * SLICE, (c + 1) * SLICE)
        w = jnp.concatenate([r[:, cols] for r in w_refs], axis=0)
        p = lax.dot_general(dd, w, dims, preferred_element_type=F32).astype(BF16)
        p = p.reshape(2, 1, TOK, SLICE)

        @pl.when(mine == c)
        def _():
            own[...] = p

        @pl.when(mine != c)
        def _():
            other[...] = p


def pair_sum_kernel(own, other, out):
    zh = lax.axis_index("zh")
    for t in range(2):
        first = jnp.bitwise_xor(zh, t) * NZL
        for zl in range(NZL):
            s = t * NZL + zl
            out[first + zl] = (own[s].astype(F32) + other[s].astype(F32)).astype(BF16)


def total_kernel(parts, out):
    total = parts[0].astype(F32)
    for n in range(1, NZ):
        total = total + parts[n].astype(F32)
    out[...] = total.astype(BF16)


def relay_kernel(left, right, from_right, from_left, left_out, right_out):
    left_out[...] = (left[...].astype(F32) + from_right[...].astype(F32)).astype(BF16)
    right_out[...] = (right[...].astype(F32) + from_left[...].astype(F32)).astype(BF16)


def stage_kernel(own_lo, own_hi, r_lo, r_hi, l_lo, l_hi, *outs):
    rows = own_lo.shape[0] // 2
    lo = own_lo[...].astype(F32) + r_lo[...].astype(F32) + l_lo[...].astype(F32)
    hi = own_hi[...].astype(F32) + r_hi[...].astype(F32) + l_hi[...].astype(F32)
    outs[0][...] = lo[:rows].astype(BF16)
    outs[1][...] = lo[rows:].astype(BF16)
    outs[2][...] = hi[:rows].astype(BF16)
    outs[3][...] = hi[rows:].astype(BF16)


def finish_kernel(*refs):
    a, b, gate, up = refs[:4], refs[4:8], refs[8], refs[9]
    ta = sum(r[...].astype(F32) for r in a) * (1.0 / GROUPS)
    tb = sum(r[...].astype(F32) for r in b) * (1.0 / GROUPS)
    gate[...] = jnp.concatenate([ta[:HALF_A], tb[:HALF_B]], axis=0)
    up[...] = jnp.concatenate([ta[HALF_A:], tb[HALF_B:]], axis=0)


def gather_plane(shard, first, second):
    near = [shard] + [shift(shard, **{first: -r}) for r in REL[1:]]
    lo = jnp.concatenate(near[:2], axis=0)
    hi = jnp.concatenate(near[2:], axis=0)
    left_lo = shift(lo, **{second: 1})
    right_lo = shift(lo, **{second: -1})
    left_hi = shift(hi, **{second: 1})
    right_hi = shift(hi, **{second: -1})
    far_lo = shift(left_lo, **{second: 1})
    far_hi = shift(right_hi, **{second: -1})
    return [lo, hi, left_lo, left_hi, right_lo, right_hi, far_lo, far_hi]


def reduce_plane(parts, first, second):
    own_lo, own_hi, left_lo, left_hi, right_lo, right_hi, far_lo, far_hi = parts
    n = far_lo.shape[0]
    from_right = shift(far_lo, **{second: -1})
    from_left = shift(far_hi, **{second: 1})
    r_hi = shift(left_hi, **{second: -1})
    l_lo = shift(right_lo, **{second: 1})
    left_lo, right_hi = call(relay_kernel, (shape(n, D), shape(n, D)))(
        left_lo, right_hi, from_right, from_left
    )
    r_lo = shift(left_lo, **{second: -1})
    l_hi = shift(right_hi, **{second: 1})
    pieces = call(stage_kernel, tuple(shape(n // 2, D) for _ in REL))(
        own_lo, own_hi, r_lo, r_hi, l_lo, l_hi
    )
    return [pieces[0]] + [shift(p, **{first: r}) for p, r in zip(pieces[1:], REL[1:])]


def body(tokens, gate_codes, gate_scales, up_codes, up_scales, cotangent):
    shard_a, shard_b = call(dequant_kernel, (shape(SHARD_A, D), shape(SHARD_B, D)))(
        gate_codes, gate_scales.T, up_codes, up_scales.T
    )
    wb = gather_plane(shard_b, "dy", "dx")
    wa = gather_plane(shard_a, "dx", "dy")

    copies = jnp.broadcast_to(tokens, (NZ, TOK, SLICE))
    mine = exchange_z(copies)
    theirs = shift(mine, dc=1)
    whole = call(join_kernel, shape(2 * TOK, D))(mine, theirs)

    cot_mine, cot_sent, pick = call(
        spread_kernel,
        (shape(TOK, WIDE), shape(TOK, WIDE), shape(GROUPS * ROWS, 2 * WIDE)),
        megabytes=24,
    )(cotangent)
    cot_partner = shift(cot_sent, dz=4)

    chunk = 1024
    grid = (D // chunk,)

    def cols(rows, width=chunk):
        return pl.BlockSpec((rows, width), lambda j: (0, j))

    def full(*dims):
        return pl.BlockSpec(dims, lambda j: (0,) * len(dims))

    def forward(w, half, lower):
        shard = 2 * half
        width = 16 * shard
        return call(
            functools.partial(forward_kernel, shard, half, lower),
            (shape(TOK, width), shape(TOK, width), shape(2 * TOK, width)),
            grid=grid,
            in_specs=[cols(2 * TOK), full(TOK, WIDE), full(TOK, WIDE)]
            + [cols(p.shape[0]) for p in w],
            out_specs=(full(TOK, width), full(TOK, width), full(2 * TOK, width)),
            scratch_shapes=[pltpu.VMEM((2 * TOK, width), F32)],
        )(whole, cot_mine, cot_partner, *w)

    def weight_grad(dd, parts):
        return call(
            weight_grad_kernel,
            tuple(shape(p.shape[0], D) for p in parts),
            grid=grid,
            in_specs=[full(*dd.shape), cols(2 * TOK)],
            out_specs=tuple(cols(p.shape[0]) for p in parts),
        )(dd, whole)

    hm_b, hp_b, dd_b = forward(wb, HALF_B, WIDE_A)
    sums_b = reduce_plane(weight_grad(dd_b, wb), "dy", "dx")
    hm_a, hp_a, dd_a = forward(wa, HALF_A, 0)
    sums_a = reduce_plane(weight_grad(dd_a, wa), "dx", "dy")
    gate_grad, up_grad = call(
        finish_kernel, (shape(ROWS, D, F32), shape(ROWS, D, F32))
    )(*sums_a, *sums_b)

    quad = pl.BlockSpec((2, 1, TOK, SLICE), lambda j: (0, j, 0, 0))
    quad_shape = jax.ShapeDtypeStruct((2, NZL, TOK, SLICE), BF16)
    own_tg, other_tg = call(
        token_grad_kernel,
        (quad_shape, quad_shape),
        megabytes=24,
        grid=(NZL,),
        in_specs=[full(2 * TOK, WIDE_A), full(2 * TOK, WIDE_B)]
        + [cols(w.shape[0], NC * SLICE) for w in wa + wb],
        out_specs=(quad, quad),
    )(dd_a, dd_b, *wa, *wb)
    cube = (NZ, TOK, SLICE)
    received = shift(other_tg, dc=1)
    blocks = call(pair_sum_kernel, jax.ShapeDtypeStruct(cube, BF16))(
        own_tg.reshape(cube), received.reshape(cube)
    )
    token_grad = call(total_kernel, shape(TOK, SLICE))(exchange_z(blocks))

    hidden_mine = jnp.concatenate([hm_a, hm_b], axis=1)
    hidden_back = shift(jnp.concatenate([hp_a, hp_b], axis=1), dz=4)
    hidden = call(collect_kernel, shape(TOK, GROUPS * ROWS))(
        hidden_mine, hidden_back, pick
    )
    return hidden, token_grad, gate_grad, up_grad


def solution(mesh):
    fine = Mesh(mesh.devices.reshape(NY, NZH, NX, NZL, NC), AXES)
    inter, intra = ("y", "zh", "x"), ("zl", "core")
    rows, toks = P(intra + inter, None), P(inter, intra)
    return jax.shard_map(
        body,
        mesh=fine,
        in_specs=(toks, rows, rows, rows, rows, toks),
        out_specs=(toks, toks, rows, rows),
        check_vma=False,
    )
```

```python
import functools
import jax
import jax.numpy as jnp
from jax import lax
from jax.experimental import pallas as pl
from jax.experimental.pallas import tpu as pltpu
from jax.sharding import Mesh, PartitionSpec as P


D = 4096
TOK = 128
SLICE = 512
ROWS = 28
BLOCK = 256
NY, NZH, NX, NZL, NC = 4, 2, 4, 4, 2
NZ = NZH * NZL
GROUPS = NY * NZH * NX
REL = (0, -1, 1, 2)
HALF_A, HALF_B = 16, 12
SHARD_A, SHARD_B = 2 * HALF_A, 2 * HALF_B
WIDE_A, WIDE_B = 16 * SHARD_A, 16 * SHARD_B
WIDE = WIDE_A + WIDE_B
F32, BF16 = jnp.float32, jnp.bfloat16


AXES = ("y", "zh", "x", "zl", "core")


def shift(value, dx=0, dy=0, dz=0, dc=0):
    pairs = []
    for y in range(NY):
        for zh in range(NZH):
            for x in range(NX):
                for zl in range(NZL):
                    for c in range(NC):
                        z = (zh * NZL + zl + dz) % NZ
                        source = (((y * NZH + zh) * NX + x) * NZL + zl) * NC + c
                        target = (
                            (((y + dy) % NY * NZH + z // NZL) * NX + (x + dx) % NX) * NZL + z % NZL
                        ) * NC + (c + dc) % NC
                        pairs.append((source, target))
    return lax.ppermute(value, AXES, pairs)


def exchange_z(value):
    return lax.all_to_all(value, ("zh", "zl"), 0, 0, tiled=True)


def call(kernel, outs, megabytes=16, **kw):
    return pl.pallas_call(
        kernel,
        out_shape=outs,
        compiler_params=pltpu.CompilerParams(vmem_limit_bytes=megabytes * 1024 * 1024),
        **kw,
    )


def shape(rows, cols, kind=BF16):
    return jax.ShapeDtypeStruct((rows, cols), kind)


VMEM = pl.BlockSpec(memory_space=pltpu.VMEM)


def dequant_kernel(*refs):
    sources, (a, b), (gc, gs, uc, us), sems = refs[:4], refs[4:6], refs[6:10], refs[10]
    copies = [
        pltpu.make_async_copy(source, target, sems.at[n])
        for n, (source, target) in enumerate(zip(sources, (gc, gs, uc, us)))
    ]
    for copy in copies:
        copy.start()
    for copy in copies:
        copy.wait()
    scales_g, scales_u = gs[...].T, us[...].T
    for n in range(D // BLOCK):
        cols = slice(n * BLOCK, (n + 1) * BLOCK)
        g = gc[:, cols].astype(F32) * scales_g[:, n : n + 1]
        u = uc[:, cols].astype(F32) * scales_u[:, n : n + 1]
        a[:, cols] = jnp.concatenate([g[:HALF_A], u[:HALF_A]], axis=0).astype(BF16)
        b[:, cols] = jnp.concatenate([g[HALF_A:], u[HALF_A:]], axis=0).astype(BF16)


def pair_kernel(first, second, out):
    n = first.shape[0]
    out[:n] = first[...]
    out[n:] = second[...]


def copies_kernel(tokens, out):
    for n in range(NZ):
        out[n] = tokens[...]


def rel_of(n):
    return jnp.where(n == 1, 3, jnp.where(n == 2, 1, jnp.where(n == 3, 2, 0)))


def one_hot(flip):
    y, zh, x = lax.axis_index("y"), lax.axis_index("zh"), lax.axis_index("x")
    half = jnp.bitwise_xor(zh, flip)
    col = lax.broadcasted_iota(jnp.int32, (1, WIDE_A), 1)
    s, r = col // SHARD_A, col % SHARD_A
    yy, xx = (y + rel_of(s // 4)) % NY, (x + rel_of(s % 4)) % NX
    a = jnp.where(r < HALF_A, ((yy * NZH + half) * NX + xx) * ROWS + r, -1)
    col = lax.broadcasted_iota(jnp.int32, (1, WIDE_B), 1)
    s, r = col // SHARD_B, col % SHARD_B
    yy, xx = (y + rel_of(s % 4)) % NY, (x + rel_of(s // 4)) % NX
    b = jnp.where(r < HALF_B, ((yy * NZH + half) * NX + xx) * ROWS + HALF_A + r, -1)
    origin = jnp.concatenate([a, b], axis=1)
    rows = lax.broadcasted_iota(jnp.int32, (GROUPS * ROWS, WIDE), 0)
    return (rows == origin).astype(F32).astype(BF16)


def spread_kernel(cot, mine, partner):
    flip = pl.program_id(0)
    out = jnp.dot(cot[...], one_hot(flip), preferred_element_type=F32).astype(BF16)

    @pl.when(flip == 0)
    def _():
        mine[...] = out

    @pl.when(flip == 1)
    def _():
        partner[...] = out


def collect_kernel(mine, partner, out, acc):
    flip = pl.program_id(0)
    source = jnp.where(flip == 0, mine[...], partner[...])
    dims = (((1,), (1,)), ((), ()))
    part = lax.dot_general(source, one_hot(flip), dims, preferred_element_type=F32)

    @pl.when(flip == 0)
    def _():
        acc[...] = part

    @pl.when(flip == 1)
    def _():
        out[...] = (acc[...] + part).astype(BF16)


def join_kernel(own, other, out):
    c, zh = lax.axis_index("core"), lax.axis_index("zh")
    for t in range(2):
        first = jnp.bitwise_xor(zh, t) * NZL
        for zl in range(NZL):
            rows = slice(t * TOK, (t + 1) * TOK)
            mine = pl.multiple_of((zl * NC + c) * SLICE, SLICE)
            theirs = pl.multiple_of((zl * NC + 1 - c) * SLICE, SLICE)
            out[rows, pl.ds(mine, SLICE)] = own[first + zl]
            out[rows, pl.ds(theirs, SLICE)] = other[first + zl]


def gating(gu, cot, shard, half):
    width = gu.shape[1]
    gate = gu
    up = pltpu.roll(gu, width - half, 1)
    sig = jax.nn.sigmoid(gate)
    act = gate * sig
    d_up = cot * act
    d_gate = cot * up * sig * (1.0 + gate * (1.0 - sig))
    first = lax.broadcasted_iota(jnp.int32, gu.shape, 1) % shard < half
    hidden = jnp.where(first, act * up, 0.0)
    both = jnp.where(first, d_gate, pltpu.roll(d_up, half, 1))
    return hidden.astype(BF16), both.astype(BF16)


def forward_kernel(shard, half, lower, x, cot_mine, cot_partner, *refs):
    w_refs, before = refs[:8], refs[8:-4]
    hidden_mine, hidden_partner, dd, acc = refs[-4:]
    step = pl.program_id(0)

    @pl.when(step == 0)
    def _():
        acc[...] = jnp.zeros_like(acc)

    dims = (((1,), (1,)), ((), ()))
    w = jnp.concatenate([r[...] for r in w_refs], axis=0)
    acc[...] += lax.dot_general(x[...], w, dims, preferred_element_type=F32)

    @pl.when(step == pl.num_programs(0) - 1)
    def _():
        width = acc.shape[1]
        for old, new in zip(before, (hidden_mine, hidden_partner)):
            new[:, :lower] = old[...]
        for rows, cot, hidden in (
            (slice(0, TOK), cot_mine, hidden_mine),
            (slice(TOK, 2 * TOK), cot_partner, hidden_partner),
        ):
            back = cot[:, lower : lower + width].astype(F32)
            h, dd[rows, :] = gating(acc[rows, :], back, shard, half)
            hidden[:, lower : lower + width] = h


def weight_grad_kernel(dd, x, *outs):
    g = lax.dot_general(dd[...], x[...], (((0,), (0,)), ((), ())), preferred_element_type=F32)
    n = outs[0].shape[0]
    for i, out in enumerate(outs):
        out[...] = g[i * n : (i + 1) * n].astype(BF16)


def token_grad_kernel(dd_a, dd_b, *refs):
    w_refs = refs[:16]
    own, other = refs[16:]
    mine = lax.axis_index("core")
    dims = (((1,), (0,)), ((), ()))
    dd = jnp.concatenate([dd_a[...], dd_b[...]], axis=1)
    c = pl.program_id(1)
    cols = pl.ds(pl.multiple_of(c * SLICE, SLICE), SLICE)
    w = jnp.concatenate([r[:, cols] for r in w_refs], axis=0)
    p = lax.dot_general(dd, w, dims, preferred_element_type=F32).astype(BF16)
    p = p.reshape(2, 1, TOK, SLICE)

    @pl.when(mine == c)
    def _():
        own[...] = p

    @pl.when(mine != c)
    def _():
        other[...] = p


def pair_sum_kernel(own, other, out):
    zh = lax.axis_index("zh")
    for t in range(2):
        first = jnp.bitwise_xor(zh, t) * NZL
        for zl in range(NZL):
            s = t * NZL + zl
            out[first + zl] = (own[s].astype(F32) + other[s].astype(F32)).astype(BF16)


def total_kernel(parts, out):
    total = parts[0].astype(F32)
    for n in range(1, NZ):
        total = total + parts[n].astype(F32)
    out[...] = total.astype(BF16)


def relay_kernel(left, right, from_right, from_left, left_out, right_out):
    left_out[...] = (left[...].astype(F32) + from_right[...].astype(F32)).astype(BF16)
    right_out[...] = (right[...].astype(F32) + from_left[...].astype(F32)).astype(BF16)


def stage_kernel(own_lo, own_hi, r_lo, r_hi, l_lo, l_hi, *outs):
    rows = own_lo.shape[0] // 2
    lo = own_lo[...].astype(F32) + r_lo[...].astype(F32) + l_lo[...].astype(F32)
    hi = own_hi[...].astype(F32) + r_hi[...].astype(F32) + l_hi[...].astype(F32)
    outs[0][...] = lo[:rows].astype(BF16)
    outs[1][...] = lo[rows:].astype(BF16)
    outs[2][...] = hi[:rows].astype(BF16)
    outs[3][...] = hi[rows:].astype(BF16)


def finish_kernel(*refs):
    a, b, gate, up = refs[:4], refs[4:8], refs[8], refs[9]
    ta = sum(r[...].astype(F32) for r in a) * (1.0 / GROUPS)
    tb = sum(r[...].astype(F32) for r in b) * (1.0 / GROUPS)
    gate[...] = jnp.concatenate([ta[:HALF_A], tb[:HALF_B]], axis=0)
    up[...] = jnp.concatenate([ta[HALF_A:], tb[HALF_B:]], axis=0)


def gather_plane(shard, first, second):
    near = [shard] + [shift(shard, **{first: -r}) for r in REL[1:]]
    two = shape(2 * shard.shape[0], D)
    lo = call(pair_kernel, two, 4)(*near[:2])
    hi = call(pair_kernel, two, 4)(*near[2:])
    left_lo = shift(lo, **{second: 1})
    right_lo = shift(lo, **{second: -1})
    left_hi = shift(hi, **{second: 1})
    right_hi = shift(hi, **{second: -1})
    far_lo = shift(left_lo, **{second: 1})
    far_hi = shift(right_hi, **{second: -1})
    return [lo, hi, left_lo, left_hi, right_lo, right_hi, far_lo, far_hi]


def reduce_plane(parts, first, second):
    own_lo, own_hi, left_lo, left_hi, right_lo, right_hi, far_lo, far_hi = parts
    n = far_lo.shape[0]
    from_right = shift(far_lo, **{second: -1})
    from_left = shift(far_hi, **{second: 1})
    r_hi = shift(left_hi, **{second: -1})
    l_lo = shift(right_lo, **{second: 1})
    left_lo, right_hi = call(relay_kernel, (shape(n, D), shape(n, D)))(
        left_lo, right_hi, from_right, from_left
    )
    r_lo = shift(left_lo, **{second: -1})
    l_hi = shift(right_hi, **{second: 1})
    pieces = call(stage_kernel, tuple(shape(n // 2, D) for _ in REL))(
        own_lo, own_hi, r_lo, r_hi, l_lo, l_hi
    )
    return [pieces[0]] + [shift(p, **{first: r}) for p, r in zip(pieces[1:], REL[1:])]


def body(tokens, gate_codes, gate_scales, up_codes, up_scales, cotangent):
    sources = (gate_codes, gate_scales.T, up_codes, up_scales.T)
    shard_a, shard_b = call(
        dequant_kernel,
        (shape(SHARD_A, D), shape(SHARD_B, D)),
        56,
        in_specs=[pl.BlockSpec(memory_space=pltpu.HBM)] * 4,
        out_specs=(VMEM, VMEM),
        scratch_shapes=[pltpu.VMEM(v.shape, v.dtype) for v in sources]
        + [pltpu.SemaphoreType.DMA((4,))],
    )(*sources)
    wa = gather_plane(shard_a, "dx", "dy")
    wb = gather_plane(shard_b, "dy", "dx")

    cube_shape = jax.ShapeDtypeStruct((NZ, TOK, SLICE), BF16)
    copies = call(copies_kernel, cube_shape, 4)(tokens)
    mine = exchange_z(copies)
    theirs = shift(mine, dc=1)
    whole = call(join_kernel, shape(2 * TOK, D), 8)(mine, theirs)

    def full(*dims):
        return pl.BlockSpec(dims, lambda *_: (0,) * len(dims))

    cot_mine, cot_sent = call(
        spread_kernel,
        (shape(TOK, WIDE), shape(TOK, WIDE)),
        grid=(2,),
        in_specs=[full(TOK, GROUPS * ROWS)],
        out_specs=(full(TOK, WIDE), full(TOK, WIDE)),
    )(cotangent)
    cot_partner = shift(cot_sent, dz=4)

    chunk = 512
    grid = (D // chunk,)

    def cols(rows, width=chunk):
        return pl.BlockSpec((rows, width), lambda j, *_: (0, j))

    def forward(w, half, lower, *before):
        shard = 2 * half
        width = 16 * shard
        total = lower + width
        return call(
            functools.partial(forward_kernel, shard, half, lower),
            (shape(TOK, total), shape(TOK, total), shape(2 * TOK, width)),
            grid=grid,
            in_specs=[cols(2 * TOK), full(TOK, WIDE), full(TOK, WIDE)]
            + [cols(p.shape[0]) for p in w]
            + [full(*p.shape) for p in before],
            out_specs=(full(TOK, total), full(TOK, total), full(2 * TOK, width)),
            scratch_shapes=[pltpu.VMEM((2 * TOK, width), F32)],
        )(whole, cot_mine, cot_partner, *w, *before)

    def weight_grad(dd, parts):
        return call(
            weight_grad_kernel,
            tuple(shape(p.shape[0], D) for p in parts),
            grid=grid,
            in_specs=[full(*dd.shape), cols(2 * TOK)],
            out_specs=tuple(cols(p.shape[0]) for p in parts),
        )(dd, whole)

    hm_a, hp_a, dd_a = forward(wa, HALF_A, 0)
    hidden_mine, hidden_sent, dd_b = forward(wb, HALF_B, WIDE_A, hm_a, hp_a)
    sums_a = reduce_plane(weight_grad(dd_a, wa), "dx", "dy")
    sums_b = reduce_plane(weight_grad(dd_b, wb), "dy", "dx")
    gate_grad, up_grad = call(
        finish_kernel, (shape(ROWS, D, F32), shape(ROWS, D, F32))
    )(*sums_a, *sums_b)

    quad = pl.BlockSpec((2, 1, TOK, SLICE), lambda j, c: (0, j, 0, 0))
    quad_shape = jax.ShapeDtypeStruct((2, NZL, TOK, SLICE), BF16)
    own_tg, other_tg = call(
        token_grad_kernel,
        (quad_shape, quad_shape),
        megabytes=24,
        grid=(NZL, NC),
        in_specs=[full(2 * TOK, WIDE_A), full(2 * TOK, WIDE_B)]
        + [cols(w.shape[0], NC * SLICE) for w in wa + wb],
        out_specs=(quad, quad),
    )(dd_a, dd_b, *wa, *wb)
    cube = (NZ, TOK, SLICE)
    received = shift(other_tg, dc=1)
    blocks = call(pair_sum_kernel, cube_shape, 8)(
        own_tg.reshape(cube), received.reshape(cube)
    )
    token_grad = call(total_kernel, shape(TOK, SLICE))(exchange_z(blocks))

    hidden = call(
        collect_kernel,
        shape(TOK, GROUPS * ROWS),
        grid=(2,),
        in_specs=[full(TOK, WIDE), full(TOK, WIDE)],
        out_specs=full(TOK, GROUPS * ROWS),
        scratch_shapes=[pltpu.VMEM((TOK, GROUPS * ROWS), F32)],
    )(hidden_mine, shift(hidden_sent, dz=4))
    return hidden, token_grad, gate_grad, up_grad


def solution(mesh):
    fine = Mesh(mesh.devices.reshape(NY, NZH, NX, NZL, NC), AXES)
    inter, intra = ("y", "zh", "x"), ("zl", "core")
    rows, toks = P(intra + inter, None), P(inter, intra)
    return jax.shard_map(
        body,
        mesh=fine,
        in_specs=(toks, rows, rows, rows, rows, toks),
        out_specs=(toks, toks, rows, rows),
        check_vma=False,
    )
```

```python
import functools
import jax
import jax.numpy as jnp
from jax import lax
from jax.experimental import pallas as pl
from jax.experimental.pallas import tpu as pltpu
from jax.sharding import Mesh, PartitionSpec as P


D = 4096
TOK = 128
SLICE = 512
WIDTH = 1024
ROWS = 28
BLOCK = 256
NY, NZH, NX, NZL, NC = 4, 2, 4, 4, 2
NZ = NZH * NZL
GROUPS = NY * NZH * NX
REL = (0, -1, 1, 2)
HALF_A, HALF_B = 16, 12
SHARD_A, SHARD_B = 2 * HALF_A, 2 * HALF_B
WIDE_A, WIDE_B = 16 * SHARD_A, 16 * SHARD_B
WIDE = WIDE_A + WIDE_B
F32, BF16 = jnp.float32, jnp.bfloat16


AXES = ("y", "zh", "x", "zl", "core")


def shift(value, dx=0, dy=0, dz=0, dc=0):
    pairs = []
    for y in range(NY):
        for zh in range(NZH):
            for x in range(NX):
                for zl in range(NZL):
                    for c in range(NC):
                        z = (zh * NZL + zl + dz) % NZ
                        source = (((y * NZH + zh) * NX + x) * NZL + zl) * NC + c
                        target = (
                            (((y + dy) % NY * NZH + z // NZL) * NX + (x + dx) % NX) * NZL + z % NZL
                        ) * NC + (c + dc) % NC
                        pairs.append((source, target))
    return lax.ppermute(value, AXES, pairs)


def exchange_z(value):
    return lax.all_to_all(value, ("zh", "zl"), 0, 0, tiled=True)


def call(kernel, outs, megabytes=16, **kw):
    return pl.pallas_call(
        kernel,
        out_shape=outs,
        compiler_params=pltpu.CompilerParams(vmem_limit_bytes=megabytes * 1024 * 1024),
        **kw,
    )


def shape(rows, cols, kind=BF16):
    return jax.ShapeDtypeStruct((rows, cols), kind)


VMEM = pl.BlockSpec(memory_space=pltpu.VMEM)


def whole_block(*dims):
    return pl.BlockSpec(dims, lambda n: (0,) * len(dims))


def dequant_kernel(*refs):
    sources, (a, b), (gc, gs, uc, us), sems = refs[:4], refs[4:6], refs[6:10], refs[10]
    copies = [
        pltpu.make_async_copy(source, target, sems.at[n])
        for n, (source, target) in enumerate(zip(sources, (gc, gs, uc, us)))
    ]
    for copy in copies:
        copy.start()
    for copy in copies:
        copy.wait()
    scales_g, scales_u = gs[...].T, us[...].T
    for n in range(D // BLOCK):
        cols = slice(n * BLOCK, (n + 1) * BLOCK)
        g = gc[:, cols].astype(F32) * scales_g[:, n : n + 1]
        u = uc[:, cols].astype(F32) * scales_u[:, n : n + 1]
        a[:, cols] = jnp.concatenate([g[:HALF_A], u[:HALF_A]], axis=0).astype(BF16)
        b[:, cols] = jnp.concatenate([g[HALF_A:], u[HALF_A:]], axis=0).astype(BF16)


def pair_kernel(first, second, out):
    n = first.shape[0]
    out[:n] = first[...]
    out[n:] = second[...]


def copies_kernel(tokens, out):
    for n in range(NZ):
        out[n] = tokens[...]


def rel_of(n):
    return jnp.where(n == 1, 3, jnp.where(n == 2, 1, jnp.where(n == 3, 2, 0)))


def one_hot(flip):
    y, zh, x = lax.axis_index("y"), lax.axis_index("zh"), lax.axis_index("x")
    half = jnp.bitwise_xor(zh, flip)
    col = lax.broadcasted_iota(jnp.int32, (1, WIDE_A), 1)
    s, r = col // SHARD_A, col % SHARD_A
    yy, xx = (y + rel_of(s // 4)) % NY, (x + rel_of(s % 4)) % NX
    a = jnp.where(r < HALF_A, ((yy * NZH + half) * NX + xx) * ROWS + r, -1)
    col = lax.broadcasted_iota(jnp.int32, (1, WIDE_B), 1)
    s, r = col // SHARD_B, col % SHARD_B
    yy, xx = (y + rel_of(s % 4)) % NY, (x + rel_of(s // 4)) % NX
    b = jnp.where(r < HALF_B, ((yy * NZH + half) * NX + xx) * ROWS + HALF_A + r, -1)
    origin = jnp.concatenate([a, b], axis=1)
    rows = lax.broadcasted_iota(jnp.int32, (GROUPS * ROWS, WIDE), 0)
    return (rows == origin).astype(F32).astype(BF16)


def spread_kernel(mine, partner, out):
    both = jnp.concatenate([mine[...], partner[...]], axis=0)
    out[...] = jnp.dot(both, one_hot(0), preferred_element_type=F32).astype(BF16)


def collect_kernel(mine, partner, out, acc):
    flip = pl.program_id(0)
    source = jnp.where(flip == 0, mine[...], partner[...])
    dims = (((1,), (1,)), ((), ()))
    part = lax.dot_general(source, one_hot(flip), dims, preferred_element_type=F32)

    @pl.when(flip == 0)
    def _():
        acc[...] = part

    @pl.when(flip == 1)
    def _():
        out[...] = (acc[...] + part).astype(BF16)


def join_kernel(own, other, out):
    c, zh = lax.axis_index("core"), lax.axis_index("zh")
    for t in range(2):
        first = jnp.bitwise_xor(zh, t) * NZL
        for zl in range(NZL):
            rows = slice(t * TOK, (t + 1) * TOK)
            mine = pl.multiple_of((zl * NC + c) * SLICE, SLICE)
            theirs = pl.multiple_of((zl * NC + 1 - c) * SLICE, SLICE)
            out[rows, pl.ds(mine, SLICE)] = own[first + zl]
            out[rows, pl.ds(theirs, SLICE)] = other[first + zl]


def gating(gu, cot, shard, half):
    width = gu.shape[1]
    gate = gu
    up = pltpu.roll(gu, width - half, 1)
    sig = jax.nn.sigmoid(gate)
    act = gate * sig
    d_up = cot * act
    d_gate = cot * up * sig * (1.0 + gate * (1.0 - sig))
    first = lax.broadcasted_iota(jnp.int32, gu.shape, 1) % shard < half
    hidden = jnp.where(first, act * up, 0.0)
    both = jnp.where(first, d_gate, pltpu.roll(d_up, half, 1))
    return hidden.astype(BF16), both.astype(BF16)


def chunk(n, width):
    return pl.ds(pl.multiple_of(n * width, width), width)


def forward_kernel(shard, half, lower, x, cot, *refs):
    w_refs, before = refs[:8], refs[8:-4]
    hidden_mine, hidden_partner, dd, acc = refs[-4:]
    dims = (((1,), (1,)), ((), ()))
    acc[...] = jnp.zeros_like(acc)

    @pl.loop(0, D // WIDTH)
    def _(n):
        cols = chunk(n, WIDTH)
        w = jnp.concatenate([r[:, cols] for r in w_refs], axis=0)
        acc[...] += lax.dot_general(x[:, cols], w, dims, preferred_element_type=F32)

    width = acc.shape[1]
    for old, new in zip(before, (hidden_mine, hidden_partner)):
        new[:, :lower] = old[...]
    back = cot[:, lower : lower + width].astype(F32)
    h, dd[...] = gating(acc[...], back, shard, half)
    hidden_mine[:, lower : lower + width] = h[:TOK]
    hidden_partner[:, lower : lower + width] = h[TOK:]


def weight_grad_kernel(dd, x, *outs):
    turned = dd[...].T
    n = outs[0].shape[0]

    @pl.loop(0, D // WIDTH)
    def _(m):
        cols = chunk(m, WIDTH)
        g = jnp.dot(turned, x[:, cols], preferred_element_type=F32)
        for i, out in enumerate(outs):
            out[:, cols] = g[i * n : (i + 1) * n].astype(BF16)


def token_grad_kernel(dd_a, dd_b, *refs):
    w_refs = refs[:16]
    own, other = refs[16:]
    mine = lax.axis_index("core")
    dd = jnp.concatenate([dd_a[...], dd_b[...]], axis=1)

    @pl.loop(0, NZL * NC)
    def _(n):
        cols = chunk(n, SLICE)
        w = jnp.concatenate([r[:, cols] for r in w_refs], axis=0)
        p = jnp.dot(dd, w, preferred_element_type=F32).astype(BF16)
        p = p.reshape(2, 1, TOK, SLICE)
        there = pl.ds(n // NC, 1)

        @pl.when(mine == n % NC)
        def _():
            own[:, there] = p

        @pl.when(mine != n % NC)
        def _():
            other[:, there] = p


def pair_sum_kernel(own, other, out):
    zh = lax.axis_index("zh")
    for t in range(2):
        first = jnp.bitwise_xor(zh, t) * NZL
        for zl in range(NZL):
            s = t * NZL + zl
            out[first + zl] = (own[s].astype(F32) + other[s].astype(F32)).astype(BF16)


def total_kernel(parts, out):
    total = parts[0].astype(F32)
    for n in range(1, NZ):
        total = total + parts[n].astype(F32)
    out[...] = total.astype(BF16)


def relay_kernel(left, right, from_right, from_left, left_out, right_out):
    left_out[...] = (left[...].astype(F32) + from_right[...].astype(F32)).astype(BF16)
    right_out[...] = (right[...].astype(F32) + from_left[...].astype(F32)).astype(BF16)


def stage_kernel(own_lo, own_hi, r_lo, r_hi, l_lo, l_hi, *outs):
    rows = own_lo.shape[0] // 2
    lo = own_lo[...].astype(F32) + r_lo[...].astype(F32) + l_lo[...].astype(F32)
    hi = own_hi[...].astype(F32) + r_hi[...].astype(F32) + l_hi[...].astype(F32)
    outs[0][...] = lo[:rows].astype(BF16)
    outs[1][...] = lo[rows:].astype(BF16)
    outs[2][...] = hi[:rows].astype(BF16)
    outs[3][...] = hi[rows:].astype(BF16)


def finish_kernel(*refs):
    a, b, gate, up = refs[:4], refs[4:8], refs[8], refs[9]
    ta = sum(r[...].astype(F32) for r in a) * (1.0 / GROUPS)
    tb = sum(r[...].astype(F32) for r in b) * (1.0 / GROUPS)
    gate[...] = jnp.concatenate([ta[:HALF_A], tb[:HALF_B]], axis=0)
    up[...] = jnp.concatenate([ta[HALF_A:], tb[HALF_B:]], axis=0)


def gather_plane(shard, first, second):
    near = [shard] + [shift(shard, **{first: -r}) for r in REL[1:]]
    two = shape(2 * shard.shape[0], D)
    lo = call(pair_kernel, two, 4)(*near[:2])
    hi = call(pair_kernel, two, 4)(*near[2:])
    left_lo = shift(lo, **{second: 1})
    right_lo = shift(lo, **{second: -1})
    left_hi = shift(hi, **{second: 1})
    right_hi = shift(hi, **{second: -1})
    far_lo = shift(left_lo, **{second: 1})
    far_hi = shift(right_hi, **{second: -1})
    return [lo, hi, left_lo, left_hi, right_lo, right_hi, far_lo, far_hi]


def reduce_plane(parts, first, second):
    own_lo, own_hi, left_lo, left_hi, right_lo, right_hi, far_lo, far_hi = parts
    n = far_lo.shape[0]
    from_right = shift(far_lo, **{second: -1})
    from_left = shift(far_hi, **{second: 1})
    r_hi = shift(left_hi, **{second: -1})
    l_lo = shift(right_lo, **{second: 1})
    left_lo, right_hi = call(relay_kernel, (shape(n, D), shape(n, D)))(
        left_lo, right_hi, from_right, from_left
    )
    r_lo = shift(left_lo, **{second: -1})
    l_hi = shift(right_hi, **{second: 1})
    pieces = call(stage_kernel, tuple(shape(n // 2, D) for _ in REL))(
        own_lo, own_hi, r_lo, r_hi, l_lo, l_hi
    )
    return [pieces[0]] + [shift(p, **{first: r}) for p, r in zip(pieces[1:], REL[1:])]


def body(tokens, gate_codes, gate_scales, up_codes, up_scales, cotangent):
    sources = (gate_codes, gate_scales.T, up_codes, up_scales.T)
    shard_a, shard_b = call(
        dequant_kernel,
        (shape(SHARD_A, D), shape(SHARD_B, D)),
        56,
        in_specs=[pl.BlockSpec(memory_space=pltpu.HBM)] * 4,
        out_specs=(VMEM, VMEM),
        scratch_shapes=[pltpu.VMEM(v.shape, v.dtype) for v in sources]
        + [pltpu.SemaphoreType.DMA((4,))],
    )(*sources)
    wa = gather_plane(shard_a, "dx", "dy")
    wb = gather_plane(shard_b, "dy", "dx")

    cube_shape = jax.ShapeDtypeStruct((NZ, TOK, SLICE), BF16)
    copies = call(copies_kernel, cube_shape, 4)(tokens)
    mine = exchange_z(copies)
    theirs = shift(mine, dc=1)
    whole = call(join_kernel, shape(2 * TOK, D), 8)(mine, theirs)

    cot = call(spread_kernel, shape(2 * TOK, WIDE))(cotangent, shift(cotangent, dz=4))

    def forward(w, half, lower, *before):
        shard = 2 * half
        width = 16 * shard
        total = lower + width
        return call(
            functools.partial(forward_kernel, shard, half, lower),
            (shape(TOK, total), shape(TOK, total), shape(2 * TOK, width)),
            scratch_shapes=[pltpu.VMEM((2 * TOK, width), F32)],
        )(whole, cot, *w, *before)

    def weight_grad(dd, parts):
        return call(weight_grad_kernel, tuple(shape(p.shape[0], D) for p in parts))(
            dd, whole
        )

    hm_a, hp_a, dd_a = forward(wa, HALF_A, 0)
    hidden_mine, hidden_sent, dd_b = forward(wb, HALF_B, WIDE_A, hm_a, hp_a)
    sums_a = reduce_plane(weight_grad(dd_a, wa), "dx", "dy")
    sums_b = reduce_plane(weight_grad(dd_b, wb), "dy", "dx")
    gate_grad, up_grad = call(
        finish_kernel, (shape(ROWS, D, F32), shape(ROWS, D, F32))
    )(*sums_a, *sums_b)

    quad = jax.ShapeDtypeStruct((2, NZL, TOK, SLICE), BF16)
    own_tg, other_tg = call(token_grad_kernel, (quad, quad), 20)(dd_a, dd_b, *wa, *wb)
    cube = (NZ, TOK, SLICE)
    received = shift(other_tg, dc=1)
    blocks = call(pair_sum_kernel, cube_shape, 8)(
        own_tg.reshape(cube), received.reshape(cube)
    )
    token_grad = call(total_kernel, shape(TOK, SLICE))(exchange_z(blocks))

    hidden = call(
        collect_kernel,
        shape(TOK, GROUPS * ROWS),
        grid=(2,),
        in_specs=[whole_block(TOK, WIDE), whole_block(TOK, WIDE)],
        out_specs=whole_block(TOK, GROUPS * ROWS),
        scratch_shapes=[pltpu.VMEM((TOK, GROUPS * ROWS), F32)],
    )(hidden_mine, shift(hidden_sent, dz=4))
    return hidden, token_grad, gate_grad, up_grad


def solution(mesh):
    fine = Mesh(mesh.devices.reshape(NY, NZH, NX, NZL, NC), AXES)
    inter, intra = ("y", "zh", "x"), ("zl", "core")
    rows, toks = P(intra + inter, None), P(inter, intra)
    return jax.shard_map(
        body,
        mesh=fine,
        in_specs=(toks, rows, rows, rows, rows, toks),
        out_specs=(toks, toks, rows, rows),
        check_vma=False,
    )
```

```python
import functools
import jax
import jax.numpy as jnp
from jax import lax
from jax.experimental import pallas as pl
from jax.experimental.pallas import tpu as pltpu
from jax.sharding import Mesh, PartitionSpec as P


D = 4096
TOK = 128
SLICE = 512
WIDTH = 1024
ROWS = 28
BLOCK = 256
NY, NZH, NX, NZL, NC = 4, 2, 4, 4, 2
NZ = NZH * NZL
GROUPS = NY * NZH * NX
REL = (0, -1, 1, 2)
HALF_A, HALF_B = 16, 12
SHARD_A, SHARD_B = 2 * HALF_A, 2 * HALF_B
WIDE_A, WIDE_B = 16 * SHARD_A, 16 * SHARD_B
WIDE = WIDE_A + WIDE_B
F32, BF16 = jnp.float32, jnp.bfloat16


AXES = ("y", "zh", "x", "zl", "core")


def shift(value, dx=0, dy=0, dz=0, dc=0):
    pairs = []
    for y in range(NY):
        for zh in range(NZH):
            for x in range(NX):
                for zl in range(NZL):
                    for c in range(NC):
                        z = (zh * NZL + zl + dz) % NZ
                        source = (((y * NZH + zh) * NX + x) * NZL + zl) * NC + c
                        target = (
                            (((y + dy) % NY * NZH + z // NZL) * NX + (x + dx) % NX) * NZL + z % NZL
                        ) * NC + (c + dc) % NC
                        pairs.append((source, target))
    return lax.ppermute(value, AXES, pairs)


def exchange_z(value):
    return lax.all_to_all(value, ("zh", "zl"), 0, 0, tiled=True)


def call(kernel, outs, megabytes=16, **kw):
    return pl.pallas_call(
        kernel,
        out_shape=outs,
        compiler_params=pltpu.CompilerParams(vmem_limit_bytes=megabytes * 1024 * 1024),
        **kw,
    )


def shape(rows, cols, kind=BF16):
    return jax.ShapeDtypeStruct((rows, cols), kind)


VMEM = pl.BlockSpec(memory_space=pltpu.VMEM)


def in_hbm(value):
    return pltpu.with_memory_space_constraint(value, pltpu.HBM)


def whole_block(*dims):
    return pl.BlockSpec(dims, lambda n: (0,) * len(dims))


def dequant_kernel(tokens, *refs):
    sources, (a, b, spread), (gc, gs, uc, us), sems = refs[:4], refs[4:7], refs[7:11], refs[11]
    pairs = list(zip(sources, (gc, gs, uc, us))) + [(tokens, spread.at[n]) for n in range(NZ)]
    copies = [
        pltpu.make_async_copy(source, target, sems.at[n])
        for n, (source, target) in enumerate(pairs)
    ]
    for copy in copies:
        copy.start()
    for copy in copies[:4]:
        copy.wait()
    scales_g, scales_u = gs[...].T, us[...].T
    for n in range(D // BLOCK):
        cols = slice(n * BLOCK, (n + 1) * BLOCK)
        g = gc[:, cols].astype(F32) * scales_g[:, n : n + 1]
        u = uc[:, cols].astype(F32) * scales_u[:, n : n + 1]
        a[:, cols] = jnp.concatenate([g[:HALF_A], u[:HALF_A]], axis=0).astype(BF16)
        b[:, cols] = jnp.concatenate([g[HALF_A:], u[HALF_A:]], axis=0).astype(BF16)
    for copy in copies[4:]:
        copy.wait()


def pair_kernel(first, second, out):
    n = first.shape[0]
    out[:n] = first[...]
    out[n:] = second[...]


def rel_of(n):
    return jnp.where(n == 1, 3, jnp.where(n == 2, 1, jnp.where(n == 3, 2, 0)))


def one_hot(flip):
    y, zh, x = lax.axis_index("y"), lax.axis_index("zh"), lax.axis_index("x")
    half = jnp.bitwise_xor(zh, flip)
    col = lax.broadcasted_iota(jnp.int32, (1, WIDE_A), 1)
    s, r = col // SHARD_A, col % SHARD_A
    yy, xx = (y + rel_of(s // 4)) % NY, (x + rel_of(s % 4)) % NX
    a = jnp.where(r < HALF_A, ((yy * NZH + half) * NX + xx) * ROWS + r, -1)
    col = lax.broadcasted_iota(jnp.int32, (1, WIDE_B), 1)
    s, r = col // SHARD_B, col % SHARD_B
    yy, xx = (y + rel_of(s % 4)) % NY, (x + rel_of(s // 4)) % NX
    b = jnp.where(r < HALF_B, ((yy * NZH + half) * NX + xx) * ROWS + HALF_A + r, -1)
    origin = jnp.concatenate([a, b], axis=1)
    rows = lax.broadcasted_iota(jnp.int32, (GROUPS * ROWS, WIDE), 0)
    return (rows == origin).astype(F32).astype(BF16)


def spread_kernel(mine, partner, out):
    both = jnp.concatenate([mine[...], partner[...]], axis=0)
    out[...] = jnp.dot(both, one_hot(0), preferred_element_type=F32).astype(BF16)


def collect_kernel(mine, partner, out, acc):
    flip = pl.program_id(0)
    source = jnp.where(flip == 0, mine[...], partner[...])
    dims = (((1,), (1,)), ((), ()))
    part = lax.dot_general(source, one_hot(flip), dims, preferred_element_type=F32)

    @pl.when(flip == 0)
    def _():
        acc[...] = part

    @pl.when(flip == 1)
    def _():
        out[...] = (acc[...] + part).astype(BF16)


def join_kernel(own, other, out):
    c, zh = lax.axis_index("core"), lax.axis_index("zh")
    for t in range(2):
        first = jnp.bitwise_xor(zh, t) * NZL
        for zl in range(NZL):
            rows = slice(t * TOK, (t + 1) * TOK)
            mine = pl.multiple_of((zl * NC + c) * SLICE, SLICE)
            theirs = pl.multiple_of((zl * NC + 1 - c) * SLICE, SLICE)
            out[rows, pl.ds(mine, SLICE)] = own[first + zl]
            out[rows, pl.ds(theirs, SLICE)] = other[first + zl]


def gating(gu, cot, shard, half):
    width = gu.shape[1]
    gate = gu
    up = pltpu.roll(gu, width - half, 1)
    sig = jax.nn.sigmoid(gate)
    act = gate * sig
    d_up = cot * act
    d_gate = cot * up * sig * (1.0 + gate * (1.0 - sig))
    first = lax.broadcasted_iota(jnp.int32, gu.shape, 1) % shard < half
    hidden = jnp.where(first, act * up, 0.0)
    both = jnp.where(first, d_gate, pltpu.roll(d_up, half, 1))
    return hidden.astype(BF16), both.astype(BF16)


def chunk(n, width):
    return pl.ds(pl.multiple_of(n * width, width), width)


def forward_kernel(shard, half, lower, x, cot, *refs):
    w_refs, before = refs[:8], refs[8:-4]
    hidden_mine, hidden_partner, dd, acc = refs[-4:]
    dims = (((1,), (1,)), ((), ()))
    acc[...] = jnp.zeros_like(acc)

    @pl.loop(0, D // WIDTH)
    def _(n):
        cols = chunk(n, WIDTH)
        w = jnp.concatenate([r[:, cols] for r in w_refs], axis=0)
        acc[...] += lax.dot_general(x[:, cols], w, dims, preferred_element_type=F32)

    width = acc.shape[1]
    for old, new in zip(before, (hidden_mine, hidden_partner)):
        new[:, :lower] = old[...]
    back = cot[:, lower : lower + width].astype(F32)
    h, dd[...] = gating(acc[...], back, shard, half)
    hidden_mine[:, lower : lower + width] = h[:TOK]
    hidden_partner[:, lower : lower + width] = h[TOK:]


def weight_grad_kernel(dd, x, *outs):
    turned = dd[...].T
    n = outs[0].shape[0]

    @pl.loop(0, D // WIDTH)
    def _(m):
        cols = chunk(m, WIDTH)
        g = jnp.dot(turned, x[:, cols], preferred_element_type=F32)
        for i, out in enumerate(outs):
            out[:, cols] = g[i * n : (i + 1) * n].astype(BF16)


def token_grad_kernel(dd_a, dd_b, *refs):
    w_refs = refs[:16]
    own, other = refs[16:]
    mine = lax.axis_index("core")
    dd = jnp.concatenate([dd_a[...], dd_b[...]], axis=1)

    @pl.loop(0, NZL * NC)
    def _(n):
        cols = chunk(n, SLICE)
        w = jnp.concatenate([r[:, cols] for r in w_refs], axis=0)
        p = jnp.dot(dd, w, preferred_element_type=F32).astype(BF16)
        p = p.reshape(2, 1, TOK, SLICE)
        there = pl.ds(n // NC, 1)

        @pl.when(mine == n % NC)
        def _():
            own[:, there] = p

        @pl.when(mine != n % NC)
        def _():
            other[:, there] = p


def pair_sum_kernel(own, other, out):
    zh = lax.axis_index("zh")
    for t in range(2):
        first = jnp.bitwise_xor(zh, t) * NZL
        for zl in range(NZL):
            s = t * NZL + zl
            out[first + zl] = (own[s].astype(F32) + other[s].astype(F32)).astype(BF16)


def total_kernel(parts, out):
    total = parts[0].astype(F32)
    for n in range(1, NZ):
        total = total + parts[n].astype(F32)
    out[...] = total.astype(BF16)


def relay_kernel(left, right, from_right, from_left, left_out, right_out):
    left_out[...] = (left[...].astype(F32) + from_right[...].astype(F32)).astype(BF16)
    right_out[...] = (right[...].astype(F32) + from_left[...].astype(F32)).astype(BF16)


def stage_kernel(own_lo, own_hi, r_lo, r_hi, l_lo, l_hi, *outs):
    rows = own_lo.shape[0] // 2
    lo = own_lo[...].astype(F32) + r_lo[...].astype(F32) + l_lo[...].astype(F32)
    hi = own_hi[...].astype(F32) + r_hi[...].astype(F32) + l_hi[...].astype(F32)
    outs[0][...] = lo[:rows].astype(BF16)
    outs[1][...] = lo[rows:].astype(BF16)
    outs[2][...] = hi[:rows].astype(BF16)
    outs[3][...] = hi[rows:].astype(BF16)


def finish_kernel(*refs):
    a, b, gate, up = refs[:4], refs[4:8], refs[8], refs[9]
    ta = sum(r[...].astype(F32) for r in a) * (1.0 / GROUPS)
    tb = sum(r[...].astype(F32) for r in b) * (1.0 / GROUPS)
    gate[...] = jnp.concatenate([ta[:HALF_A], tb[:HALF_B]], axis=0)
    up[...] = jnp.concatenate([ta[HALF_A:], tb[HALF_B:]], axis=0)


def gather_plane(shard, first, second):
    near = [shard] + [shift(shard, **{first: -r}) for r in REL[1:]]
    two = shape(2 * shard.shape[0], D)
    lo = call(pair_kernel, two, 4)(*near[:2])
    hi = call(pair_kernel, two, 4)(*near[2:])
    left_lo = shift(lo, **{second: 1})
    right_lo = shift(lo, **{second: -1})
    left_hi = shift(hi, **{second: 1})
    right_hi = shift(hi, **{second: -1})
    far_lo = shift(left_lo, **{second: 1})
    far_hi = shift(right_hi, **{second: -1})
    return [lo, hi, left_lo, left_hi, right_lo, right_hi, far_lo, far_hi]


def reduce_plane(parts, first, second):
    own_lo, own_hi, left_lo, left_hi, right_lo, right_hi, far_lo, far_hi = parts
    n = far_lo.shape[0]
    from_right = shift(far_lo, **{second: -1})
    from_left = shift(far_hi, **{second: 1})
    r_hi = shift(left_hi, **{second: -1})
    l_lo = shift(right_lo, **{second: 1})
    left_lo, right_hi = call(relay_kernel, (shape(n, D), shape(n, D)))(
        left_lo, right_hi, from_right, from_left
    )
    r_lo = shift(left_lo, **{second: -1})
    l_hi = shift(right_hi, **{second: 1})
    pieces = call(stage_kernel, tuple(shape(n // 2, D) for _ in REL))(
        own_lo, own_hi, r_lo, r_hi, l_lo, l_hi
    )
    return [pieces[0]] + [shift(p, **{first: r}) for p, r in zip(pieces[1:], REL[1:])]


def body(tokens, gate_codes, gate_scales, up_codes, up_scales, cotangent):
    sources = (gate_codes, gate_scales.T, up_codes, up_scales.T)
    cube_shape = jax.ShapeDtypeStruct((NZ, TOK, SLICE), BF16)
    hbm = pl.BlockSpec(memory_space=pltpu.HBM)
    shard_a, shard_b, copies = call(
        dequant_kernel,
        (shape(SHARD_A, D), shape(SHARD_B, D), cube_shape),
        4,
        in_specs=[hbm] * 5,
        out_specs=(VMEM, VMEM, hbm),
        scratch_shapes=[pltpu.VMEM(v.shape, v.dtype) for v in sources]
        + [pltpu.SemaphoreType.DMA((4 + NZ,))],
    )(in_hbm(tokens), *[in_hbm(v) for v in sources])
    wa = gather_plane(shard_a, "dx", "dy")
    wb = gather_plane(shard_b, "dy", "dx")

    mine = exchange_z(copies)
    theirs = shift(mine, dc=1)
    whole = call(join_kernel, shape(2 * TOK, D), 8)(mine, theirs)

    cot = call(spread_kernel, shape(2 * TOK, WIDE))(cotangent, shift(cotangent, dz=4))

    def forward(w, half, lower, *before):
        shard = 2 * half
        width = 16 * shard
        total = lower + width
        return call(
            functools.partial(forward_kernel, shard, half, lower),
            (shape(TOK, total), shape(TOK, total), shape(2 * TOK, width)),
            scratch_shapes=[pltpu.VMEM((2 * TOK, width), F32)],
        )(whole, cot, *w, *before)

    def weight_grad(dd, parts):
        return call(weight_grad_kernel, tuple(shape(p.shape[0], D) for p in parts))(
            dd, whole
        )

    hm_a, hp_a, dd_a = forward(wa, HALF_A, 0)
    hidden_mine, hidden_sent, dd_b = forward(wb, HALF_B, WIDE_A, hm_a, hp_a)
    sums_a = reduce_plane(weight_grad(dd_a, wa), "dx", "dy")
    sums_b = reduce_plane(weight_grad(dd_b, wb), "dy", "dx")
    gate_grad, up_grad = call(
        finish_kernel, (shape(ROWS, D, F32), shape(ROWS, D, F32))
    )(*sums_a, *sums_b)

    quad = jax.ShapeDtypeStruct((2, NZL, TOK, SLICE), BF16)
    own_tg, other_tg = call(token_grad_kernel, (quad, quad), 20)(dd_a, dd_b, *wa, *wb)
    cube = (NZ, TOK, SLICE)
    received = shift(other_tg, dc=1)
    blocks = call(pair_sum_kernel, cube_shape, 8)(
        own_tg.reshape(cube), received.reshape(cube)
    )
    token_grad = call(total_kernel, shape(TOK, SLICE))(exchange_z(blocks))

    hidden = call(
        collect_kernel,
        shape(TOK, GROUPS * ROWS),
        grid=(2,),
        in_specs=[whole_block(TOK, WIDE), whole_block(TOK, WIDE)],
        out_specs=whole_block(TOK, GROUPS * ROWS),
        scratch_shapes=[pltpu.VMEM((TOK, GROUPS * ROWS), F32)],
    )(hidden_mine, shift(hidden_sent, dz=4))
    return hidden, token_grad, gate_grad, up_grad


def solution(mesh):
    fine = Mesh(mesh.devices.reshape(NY, NZH, NX, NZL, NC), AXES)
    inter, intra = ("y", "zh", "x"), ("zl", "core")
    rows, toks = P(intra + inter, None), P(inter, intra)
    return jax.shard_map(
        body,
        mesh=fine,
        in_specs=(toks, rows, rows, rows, rows, toks),
        out_specs=(toks, toks, rows, rows),
        check_vma=False,
    )
```

```python
import functools
import jax
import jax.numpy as jnp
from jax import lax
from jax.experimental import pallas as pl
from jax.experimental.pallas import tpu as pltpu
from jax.sharding import Mesh, PartitionSpec as P


D = 4096
TOK = 128
SLICE = 512
WIDTH = 1024
ROWS = 28
BLOCK = 256
NY, NZH, NX, NZL, NC = 4, 2, 4, 4, 2
NZ = NZH * NZL
GROUPS = NY * NZH * NX
HALF = NX * ROWS
REL = (0, -1, 1, 2)
HALF_A, HALF_B = 16, 12
SHARD_A, SHARD_B = 2 * HALF_A, 2 * HALF_B
WIDE_A, WIDE_B = 16 * SHARD_A, 16 * SHARD_B
WIDE = WIDE_A + WIDE_B
F32, BF16 = jnp.float32, jnp.bfloat16


AXES = ("y", "zh", "x", "zl", "core")


def shift(value, dx=0, dy=0, dz=0, dc=0):
    pairs = []
    for y in range(NY):
        for zh in range(NZH):
            for x in range(NX):
                for zl in range(NZL):
                    for c in range(NC):
                        z = (zh * NZL + zl + dz) % NZ
                        source = (((y * NZH + zh) * NX + x) * NZL + zl) * NC + c
                        target = (
                            (((y + dy) % NY * NZH + z // NZL) * NX + (x + dx) % NX) * NZL + z % NZL
                        ) * NC + (c + dc) % NC
                        pairs.append((source, target))
    return lax.ppermute(value, AXES, pairs)


def exchange_z(value):
    return lax.all_to_all(value, ("zh", "zl"), 0, 0, tiled=True)


def call(kernel, outs, megabytes=16, **kw):
    return pl.pallas_call(
        kernel,
        out_shape=outs,
        compiler_params=pltpu.CompilerParams(vmem_limit_bytes=megabytes * 1024 * 1024),
        **kw,
    )


def shape(rows, cols, kind=BF16):
    return jax.ShapeDtypeStruct((rows, cols), kind)


VMEM = pl.BlockSpec(memory_space=pltpu.VMEM)


def in_hbm(value):
    return pltpu.with_memory_space_constraint(value, pltpu.HBM)


def whole_block(*dims):
    return pl.BlockSpec(dims, lambda n: (0,) * len(dims))


def dequant_kernel(tokens, cot, *refs):
    sources, (a, b, spread, sent), scratch, sems = refs[:4], refs[4:8], refs[8:14], refs[14]
    gc, gs, uc, us, toks, back = scratch
    inputs = [
        pltpu.make_async_copy(source, target, sems.at[n])
        for n, (source, target) in enumerate(zip((*sources, tokens, cot), scratch))
    ]
    copies = [pltpu.make_async_copy(toks, spread.at[n], sems.at[6 + n]) for n in range(NZ)]
    for copy in inputs:
        copy.start()
    inputs[4].wait()
    for copy in copies:
        copy.start()
    for copy in inputs[:4]:
        copy.wait()
    scales_g, scales_u = gs[...].T, us[...].T
    for n in range(D // BLOCK):
        cols = slice(n * BLOCK, (n + 1) * BLOCK)
        g = gc[:, cols].astype(F32) * scales_g[:, n : n + 1]
        u = uc[:, cols].astype(F32) * scales_u[:, n : n + 1]
        a[:, cols] = jnp.concatenate([g[:HALF_A], u[:HALF_A]], axis=0).astype(BF16)
        b[:, cols] = jnp.concatenate([g[HALF_A:], u[HALF_A:]], axis=0).astype(BF16)
    inputs[5].wait()
    even, odd = (
        jnp.concatenate(
            [back[:, (2 * n + half) * HALF : (2 * n + half + 1) * HALF] for n in range(NY)], axis=1
        )
        for half in range(NZH)
    )
    sent[...] = jnp.where(lax.axis_index("zh") == 0, odd, even)
    for copy in copies:
        copy.wait()


def pair_kernel(first, second, out):
    n = first.shape[0]
    out[:n] = first[...]
    out[n:] = second[...]


def rel_of(n):
    return jnp.where(n == 1, 3, jnp.where(n == 2, 1, jnp.where(n == 3, 2, 0)))


def one_hot(flip, compact=False):
    y, zh, x = lax.axis_index("y"), lax.axis_index("zh"), lax.axis_index("x")
    halves = 1 if compact else NZH
    half = 0 if compact else jnp.bitwise_xor(zh, flip)
    col = lax.broadcasted_iota(jnp.int32, (1, WIDE_A), 1)
    s, r = col // SHARD_A, col % SHARD_A
    yy, xx = (y + rel_of(s // 4)) % NY, (x + rel_of(s % 4)) % NX
    a = jnp.where(r < HALF_A, ((yy * halves + half) * NX + xx) * ROWS + r, -1)
    col = lax.broadcasted_iota(jnp.int32, (1, WIDE_B), 1)
    s, r = col // SHARD_B, col % SHARD_B
    yy, xx = (y + rel_of(s % 4)) % NY, (x + rel_of(s // 4)) % NX
    b = jnp.where(r < HALF_B, ((yy * halves + half) * NX + xx) * ROWS + HALF_A + r, -1)
    origin = jnp.concatenate([a, b], axis=1)
    rows = lax.broadcasted_iota(jnp.int32, (NY * halves * HALF, WIDE), 0)
    return (rows == origin).astype(F32).astype(BF16)


def spread_kernel(mine, partner, out):
    out[:TOK] = jnp.dot(mine[...], one_hot(0), preferred_element_type=F32).astype(BF16)
    out[TOK:] = jnp.dot(partner[...], one_hot(0, True), preferred_element_type=F32).astype(BF16)


def collect_kernel(mine, partner, out, acc):
    flip = pl.program_id(0)
    source = jnp.where(flip == 0, mine[...], partner[...])
    dims = (((1,), (1,)), ((), ()))
    part = lax.dot_general(source, one_hot(flip), dims, preferred_element_type=F32)

    @pl.when(flip == 0)
    def _():
        acc[...] = part

    @pl.when(flip == 1)
    def _():
        out[...] = (acc[...] + part).astype(BF16)


def join_kernel(own, other, out):
    c, zh = lax.axis_index("core"), lax.axis_index("zh")
    for t in range(2):
        first = jnp.bitwise_xor(zh, t) * NZL
        for zl in range(NZL):
            rows = slice(t * TOK, (t + 1) * TOK)
            mine = pl.multiple_of((zl * NC + c) * SLICE, SLICE)
            theirs = pl.multiple_of((zl * NC + 1 - c) * SLICE, SLICE)
            out[rows, pl.ds(mine, SLICE)] = own[first + zl]
            out[rows, pl.ds(theirs, SLICE)] = other[first + zl]


def gating(gu, cot, shard, half):
    width = gu.shape[1]
    gate = gu
    up = pltpu.roll(gu, width - half, 1)
    sig = jax.nn.sigmoid(gate)
    act = gate * sig
    d_up = cot * act
    d_gate = cot * up * sig * (1.0 + gate * (1.0 - sig))
    first = lax.broadcasted_iota(jnp.int32, gu.shape, 1) % shard < half
    hidden = jnp.where(first, act * up, 0.0)
    both = jnp.where(first, d_gate, pltpu.roll(d_up, half, 1))
    return hidden.astype(BF16), both.astype(BF16)


def chunk(n, width):
    return pl.ds(pl.multiple_of(n * width, width), width)


def forward_kernel(shard, half, lower, x, cot, *refs):
    w_refs, before = refs[:8], refs[8:-4]
    hidden_mine, hidden_partner, dd, acc = refs[-4:]
    dims = (((1,), (1,)), ((), ()))
    acc[...] = jnp.zeros_like(acc)

    @pl.loop(0, D // WIDTH)
    def _(n):
        cols = chunk(n, WIDTH)
        w = jnp.concatenate([r[:, cols] for r in w_refs], axis=0)
        acc[...] += lax.dot_general(x[:, cols], w, dims, preferred_element_type=F32)

    width = acc.shape[1]
    for old, new in zip(before, (hidden_mine, hidden_partner)):
        new[:, :lower] = old[...]
    back = cot[:, lower : lower + width].astype(F32)
    h, dd[...] = gating(acc[...], back, shard, half)
    hidden_mine[:, lower : lower + width] = h[:TOK]
    hidden_partner[:, lower : lower + width] = h[TOK:]


def weight_grad_kernel(dd, x, *outs):
    turned = dd[...].T
    n = outs[0].shape[0]

    @pl.loop(0, D // WIDTH)
    def _(m):
        cols = chunk(m, WIDTH)
        g = jnp.dot(turned, x[:, cols], preferred_element_type=F32)
        for i, out in enumerate(outs):
            out[:, cols] = g[i * n : (i + 1) * n].astype(BF16)


def token_grad_kernel(dd_a, dd_b, *refs):
    w_refs = refs[:16]
    own, other = refs[16:]
    mine = lax.axis_index("core")
    dd = jnp.concatenate([dd_a[...], dd_b[...]], axis=1)

    @pl.loop(0, NZL * NC)
    def _(n):
        cols = chunk(n, SLICE)
        w = jnp.concatenate([r[:, cols] for r in w_refs], axis=0)
        p = jnp.dot(dd, w, preferred_element_type=F32).astype(BF16)
        p = p.reshape(2, 1, TOK, SLICE)
        there = pl.ds(n // NC, 1)

        @pl.when(mine == n % NC)
        def _():
            own[:, there] = p

        @pl.when(mine != n % NC)
        def _():
            other[:, there] = p


def pair_sum_kernel(own, other, out):
    zh = lax.axis_index("zh")
    for t in range(2):
        first = jnp.bitwise_xor(zh, t) * NZL
        for zl in range(NZL):
            s = t * NZL + zl
            out[first + zl] = (own[s].astype(F32) + other[s].astype(F32)).astype(BF16)


def total_kernel(parts, out):
    total = parts[0].astype(F32)
    for n in range(1, NZ):
        total = total + parts[n].astype(F32)
    out[...] = total.astype(BF16)


def stage_kernel(own, right, left, far, *outs):
    rows = own.shape[0] // 4
    for n, out in enumerate(outs):
        part = slice(n * rows, (n + 1) * rows)
        total = own[part].astype(F32) + right[part].astype(F32)
        total = total + (left[part].astype(F32) + far[part].astype(F32))
        out[...] = total.astype(BF16)


def finish_kernel(*refs):
    a, b, gate, up = refs[:4], refs[4:8], refs[8], refs[9]
    ta = sum(r[...].astype(F32) for r in a) * (1.0 / GROUPS)
    tb = sum(r[...].astype(F32) for r in b) * (1.0 / GROUPS)
    gate[...] = jnp.concatenate([ta[:HALF_A], tb[:HALF_B]], axis=0)
    up[...] = jnp.concatenate([ta[HALF_A:], tb[HALF_B:]], axis=0)


def gather_plane(shard, first, second):
    near = [shard] + [shift(shard, **{first: -r}) for r in REL[1:]]
    two = shape(2 * shard.shape[0], D)
    lo = call(pair_kernel, two, 4)(*near[:2])
    hi = call(pair_kernel, two, 4)(*near[2:])
    left_lo = shift(lo, **{second: 1})
    right_lo = shift(lo, **{second: -1})
    left_hi = shift(hi, **{second: 1})
    right_hi = shift(hi, **{second: -1})
    far_lo = shift(left_lo, **{second: 1})
    far_hi = shift(right_hi, **{second: -1})
    return [lo, hi, left_lo, left_hi, right_lo, right_hi, far_lo, far_hi]


def reduce_plane(parts, first, second):
    arrived = [parts[0]] + [shift(p, **{second: r}) for p, r in zip(parts[1:], REL[1:])]
    rows = parts[0].shape[0] // 4
    pieces = call(stage_kernel, tuple(shape(rows, D) for _ in REL))(*arrived)
    return [pieces[0]] + [shift(p, **{first: r}) for p, r in zip(pieces[1:], REL[1:])]


def body(tokens, gate_codes, gate_scales, up_codes, up_scales, cotangent):
    sources = (gate_codes, gate_scales.T, up_codes, up_scales.T)
    cube_shape = jax.ShapeDtypeStruct((NZ, TOK, SLICE), BF16)
    hbm = pl.BlockSpec(memory_space=pltpu.HBM)
    inputs = sources + (tokens, cotangent)
    shard_a, shard_b, copies, cot_sent = call(
        dequant_kernel,
        (shape(SHARD_A, D), shape(SHARD_B, D), cube_shape, shape(TOK, NY * HALF)),
        8,
        in_specs=[hbm] * 6,
        out_specs=(VMEM, VMEM, hbm, VMEM),
        scratch_shapes=[pltpu.VMEM(v.shape, v.dtype) for v in inputs]
        + [pltpu.SemaphoreType.DMA((len(inputs) + NZ,))],
    )(in_hbm(tokens), in_hbm(cotangent), *[in_hbm(v) for v in sources])
    wa = gather_plane(shard_a, "dx", "dy")
    wb = gather_plane(shard_b, "dy", "dx")

    mine = exchange_z(copies)
    theirs = shift(mine, dc=1)
    whole = call(join_kernel, shape(2 * TOK, D), 8)(mine, theirs)

    cot = call(spread_kernel, shape(2 * TOK, WIDE))(cotangent, shift(cot_sent, dz=4))

    def forward(w, half, lower, *before):
        shard = 2 * half
        width = 16 * shard
        total = lower + width
        return call(
            functools.partial(forward_kernel, shard, half, lower),
            (shape(TOK, total), shape(TOK, total), shape(2 * TOK, width)),
            scratch_shapes=[pltpu.VMEM((2 * TOK, width), F32)],
        )(whole, cot, *w, *before)

    def weight_grad(dd):
        outs = tuple(shape(dd.shape[1] // 4, D) for _ in REL)
        return call(weight_grad_kernel, outs)(dd, whole)

    hm_a, hp_a, dd_a = forward(wa, HALF_A, 0)
    hidden_mine, hidden_sent, dd_b = forward(wb, HALF_B, WIDE_A, hm_a, hp_a)
    sums_a = reduce_plane(weight_grad(dd_a), "dx", "dy")
    sums_b = reduce_plane(weight_grad(dd_b), "dy", "dx")
    gate_grad, up_grad = call(
        finish_kernel, (shape(ROWS, D, F32), shape(ROWS, D, F32))
    )(*sums_a, *sums_b)

    quad = jax.ShapeDtypeStruct((2, NZL, TOK, SLICE), BF16)
    own_tg, other_tg = call(token_grad_kernel, (quad, quad), 20)(
        dd_a, dd_b, *wa, *wb
    )
    cube = (NZ, TOK, SLICE)
    received = shift(other_tg, dc=1)
    blocks = call(pair_sum_kernel, cube_shape, 8)(own_tg.reshape(cube), received.reshape(cube))
    token_grad = call(total_kernel, shape(TOK, SLICE))(exchange_z(blocks))

    hidden = call(
        collect_kernel,
        shape(TOK, GROUPS * ROWS),
        grid=(2,),
        in_specs=[whole_block(TOK, WIDE), whole_block(TOK, WIDE)],
        out_specs=whole_block(TOK, GROUPS * ROWS),
        scratch_shapes=[pltpu.VMEM((TOK, GROUPS * ROWS), F32)],
    )(hidden_mine, shift(hidden_sent, dz=4))
    return hidden, token_grad, gate_grad, up_grad


def solution(mesh):
    fine = Mesh(mesh.devices.reshape(NY, NZH, NX, NZL, NC), AXES)
    inter, intra = ("y", "zh", "x"), ("zl", "core")
    rows, toks = P(intra + inter, None), P(inter, intra)
    return jax.shard_map(
        body,
        mesh=fine,
        in_specs=(toks, rows, rows, rows, rows, toks),
        out_specs=(toks, toks, rows, rows),
        check_vma=False,
    )
```

```python
import functools
import jax
import jax.numpy as jnp
from jax import lax
from jax.experimental import pallas as pl
from jax.experimental.pallas import tpu as pltpu
from jax.sharding import Mesh, PartitionSpec as P


D = 4096
TOK = 128
SLICE = 512
WIDTH = 1024
ROWS = 28
BLOCK = 256
NY, NZH, NX, NZL, NC = 4, 2, 4, 4, 2
NZ = NZH * NZL
GROUPS = NY * NZH * NX
HALF = NX * ROWS
REL = (0, -1, 1, 2)
HALF_A, HALF_B = 16, 12
SHARD_A, SHARD_B = 2 * HALF_A, 2 * HALF_B
WIDE_A, WIDE_B = 16 * SHARD_A, 16 * SHARD_B
WIDE = WIDE_A + WIDE_B
F32, BF16 = jnp.float32, jnp.bfloat16


AXES = ("y", "zh", "x", "zl", "core")


def shift(value, dx=0, dy=0, dz=0, dc=0):
    pairs = []
    for y in range(NY):
        for zh in range(NZH):
            for x in range(NX):
                for zl in range(NZL):
                    for c in range(NC):
                        z = (zh * NZL + zl + dz) % NZ
                        source = (((y * NZH + zh) * NX + x) * NZL + zl) * NC + c
                        target = (
                            (((y + dy) % NY * NZH + z // NZL) * NX + (x + dx) % NX) * NZL + z % NZL
                        ) * NC + (c + dc) % NC
                        pairs.append((source, target))
    return lax.ppermute(value, AXES, pairs)


def exchange_z(value):
    return lax.all_to_all(value, ("zh", "zl"), 0, 0, tiled=True)


def call(kernel, outs, megabytes=16, **kw):
    return pl.pallas_call(
        kernel,
        out_shape=outs,
        compiler_params=pltpu.CompilerParams(vmem_limit_bytes=megabytes * 1024 * 1024),
        **kw,
    )


def shape(rows, cols, kind=BF16):
    return jax.ShapeDtypeStruct((rows, cols), kind)


VMEM = pl.BlockSpec(memory_space=pltpu.VMEM)


def in_hbm(value):
    return pltpu.with_memory_space_constraint(value, pltpu.HBM)


def whole_block(*dims):
    return pl.BlockSpec(dims, lambda n: (0,) * len(dims))


def dequant_kernel(tokens, cot, *refs):
    sources, (a, b, spread, sent), scratch, sems = refs[:4], refs[4:8], refs[8:14], refs[14]
    gc, gs, uc, us, toks, back = scratch
    inputs = [
        pltpu.make_async_copy(source, target, sems.at[n])
        for n, (source, target) in enumerate(zip((*sources, tokens, cot), scratch))
    ]
    copies = [pltpu.make_async_copy(toks, spread.at[n], sems.at[6 + n]) for n in range(NZ)]
    for copy in inputs:
        copy.start()
    inputs[4].wait()
    for copy in copies:
        copy.start()
    for copy in inputs[:4]:
        copy.wait()
    scales_g, scales_u = gs[...].T, us[...].T
    for n in range(D // BLOCK):
        cols = slice(n * BLOCK, (n + 1) * BLOCK)
        g = gc[:, cols].astype(F32) * scales_g[:, n : n + 1]
        u = uc[:, cols].astype(F32) * scales_u[:, n : n + 1]
        a[:, cols] = jnp.concatenate([g[:HALF_A], u[:HALF_A]], axis=0).astype(BF16)
        b[:, cols] = jnp.concatenate([g[HALF_A:], u[HALF_A:]], axis=0).astype(BF16)
    inputs[5].wait()
    even, odd = (
        jnp.concatenate(
            [back[:, (2 * n + half) * HALF : (2 * n + half + 1) * HALF] for n in range(NY)], axis=1
        )
        for half in range(NZH)
    )
    sent[...] = jnp.where(lax.axis_index("zh") == 0, odd, even)
    for copy in copies:
        copy.wait()


def pair_kernel(first, second, out):
    n = first.shape[0]
    out[:n] = first[...]
    out[n:] = second[...]


def rel_of(n):
    return jnp.where(n == 1, 3, jnp.where(n == 2, 1, jnp.where(n == 3, 2, 0)))


def one_hot(flip, compact=False):
    y, zh, x = lax.axis_index("y"), lax.axis_index("zh"), lax.axis_index("x")
    halves = 1 if compact else NZH
    half = 0 if compact else jnp.bitwise_xor(zh, flip)
    col = lax.broadcasted_iota(jnp.int32, (1, WIDE_A), 1)
    s, r = col // SHARD_A, col % SHARD_A
    yy, xx = (y + rel_of(s // 4)) % NY, (x + rel_of(s % 4)) % NX
    a = jnp.where(r < HALF_A, ((yy * halves + half) * NX + xx) * ROWS + r, -1)
    col = lax.broadcasted_iota(jnp.int32, (1, WIDE_B), 1)
    s, r = col // SHARD_B, col % SHARD_B
    yy, xx = (y + rel_of(s % 4)) % NY, (x + rel_of(s // 4)) % NX
    b = jnp.where(r < HALF_B, ((yy * halves + half) * NX + xx) * ROWS + HALF_A + r, -1)
    origin = jnp.concatenate([a, b], axis=1)
    rows = lax.broadcasted_iota(jnp.int32, (NY * halves * HALF, WIDE), 0)
    return (rows == origin).astype(F32).astype(BF16)


def spread_kernel(mine, partner, out):
    out[:TOK] = jnp.dot(mine[...], one_hot(0), preferred_element_type=F32).astype(BF16)
    out[TOK:] = jnp.dot(partner[...], one_hot(0, True), preferred_element_type=F32).astype(BF16)


def collect_kernel(mine, partner, out, acc):
    flip = pl.program_id(0)
    source = jnp.where(flip == 0, mine[...], partner[...])
    dims = (((1,), (1,)), ((), ()))
    part = lax.dot_general(source, one_hot(flip), dims, preferred_element_type=F32)

    @pl.when(flip == 0)
    def _():
        acc[...] = part

    @pl.when(flip == 1)
    def _():
        out[...] = (acc[...] + part).astype(BF16)


def join_kernel(own, other, out):
    c, zh = lax.axis_index("core"), lax.axis_index("zh")
    for t in range(2):
        first = jnp.bitwise_xor(zh, t) * NZL
        for zl in range(NZL):
            rows = slice(t * TOK, (t + 1) * TOK)
            mine = pl.multiple_of((zl * NC + c) * SLICE, SLICE)
            theirs = pl.multiple_of((zl * NC + 1 - c) * SLICE, SLICE)
            out[rows, pl.ds(mine, SLICE)] = own[first + zl]
            out[rows, pl.ds(theirs, SLICE)] = other[first + zl]


def gating(gu, cot, shard, half):
    width = gu.shape[1]
    gate = gu
    up = pltpu.roll(gu, width - half, 1)
    sig = jax.nn.sigmoid(gate)
    act = gate * sig
    d_up = cot * act
    d_gate = cot * up * sig * (1.0 + gate * (1.0 - sig))
    first = lax.broadcasted_iota(jnp.int32, gu.shape, 1) % shard < half
    hidden = jnp.where(first, act * up, 0.0)
    both = jnp.where(first, d_gate, pltpu.roll(d_up, half, 1))
    return hidden.astype(BF16), both.astype(BF16)


def chunk(n, width):
    return pl.ds(pl.multiple_of(n * width, width), width)


def forward_kernel(shard, half, lower, x, cot, *refs):
    w_refs, before = refs[:8], refs[8:-4]
    hidden_mine, hidden_partner, dd, acc = refs[-4:]
    dims = (((1,), (1,)), ((), ()))
    acc[...] = jnp.zeros_like(acc)

    @pl.loop(0, D // WIDTH)
    def _(n):
        cols = chunk(n, WIDTH)
        w = jnp.concatenate([r[:, cols] for r in w_refs], axis=0)
        acc[...] += lax.dot_general(x[:, cols], w, dims, preferred_element_type=F32)

    width = acc.shape[1]
    for old, new in zip(before, (hidden_mine, hidden_partner)):
        new[:, :lower] = old[...]
    back = cot[:, lower : lower + width].astype(F32)
    h, dd[...] = gating(acc[...], back, shard, half)
    hidden_mine[:, lower : lower + width] = h[:TOK]
    hidden_partner[:, lower : lower + width] = h[TOK:]


def weight_grad_kernel(dd, x, *outs):
    turned = dd[...].T
    n = outs[0].shape[0]

    @pl.loop(0, D // WIDTH)
    def _(m):
        cols = chunk(m, WIDTH)
        g = jnp.dot(turned, x[:, cols], preferred_element_type=F32)
        for i, out in enumerate(outs):
            out[:, cols] = g[i * n : (i + 1) * n].astype(BF16)


def token_grad_kernel(dd_a, dd_b, *refs):
    w_refs = refs[:16]
    own, other = refs[16:]
    mine = lax.axis_index("core")
    dd = jnp.concatenate([dd_a[...], dd_b[...]], axis=1)

    @pl.loop(0, NZL * NC)
    def _(n):
        cols = chunk(n, SLICE)
        w = jnp.concatenate([r[:, cols] for r in w_refs], axis=0)
        p = jnp.dot(dd, w, preferred_element_type=F32).astype(BF16)
        p = p.reshape(2, 1, TOK, SLICE)
        there = pl.ds(n // NC, 1)

        @pl.when(mine == n % NC)
        def _():
            own[:, there] = p

        @pl.when(mine != n % NC)
        def _():
            other[:, there] = p


def pair_sum_kernel(own, other, out):
    zh = lax.axis_index("zh")
    for t in range(2):
        first = jnp.bitwise_xor(zh, t) * NZL
        for zl in range(NZL):
            s = t * NZL + zl
            out[first + zl] = (own[s].astype(F32) + other[s].astype(F32)).astype(BF16)


def stage_kernel(own, right, left, far, *outs):
    rows = own.shape[0] // 4
    for n, out in enumerate(outs):
        part = slice(n * rows, (n + 1) * rows)
        total = own[part].astype(F32) + right[part].astype(F32)
        total = total + (left[part].astype(F32) + far[part].astype(F32))
        out[...] = total.astype(BF16)


def relay_kernel(left, right, from_right, from_left, left_out, right_out):
    left_out[...] = (left[...].astype(F32) + from_right[...].astype(F32)).astype(BF16)
    right_out[...] = (right[...].astype(F32) + from_left[...].astype(F32)).astype(BF16)


def halves_kernel(own_lo, own_hi, r_lo, r_hi, l_lo, l_hi, *outs):
    rows = own_lo.shape[0] // 2
    lo = own_lo[...].astype(F32) + r_lo[...].astype(F32) + l_lo[...].astype(F32)
    hi = own_hi[...].astype(F32) + r_hi[...].astype(F32) + l_hi[...].astype(F32)
    outs[0][...] = lo[:rows].astype(BF16)
    outs[1][...] = lo[rows:].astype(BF16)
    outs[2][...] = hi[:rows].astype(BF16)
    outs[3][...] = hi[rows:].astype(BF16)


def finish_kernel(*refs):
    a, b, parts, gate, up, token_grad = refs[:4], refs[4:8], *refs[8:]
    total = parts[0].astype(F32)
    for n in range(1, NZ):
        total = total + parts[n].astype(F32)
    token_grad[...] = total.astype(BF16)
    ta = sum(r[...].astype(F32) for r in a) * (1.0 / GROUPS)
    tb = sum(r[...].astype(F32) for r in b) * (1.0 / GROUPS)
    gate[...] = jnp.concatenate([ta[:HALF_A], tb[:HALF_B]], axis=0)
    up[...] = jnp.concatenate([ta[HALF_A:], tb[HALF_B:]], axis=0)


def gather_plane(shard, first, second):
    near = [shard] + [shift(shard, **{first: -r}) for r in REL[1:]]
    two = shape(2 * shard.shape[0], D)
    lo = call(pair_kernel, two, 4)(*near[:2])
    hi = call(pair_kernel, two, 4)(*near[2:])
    left_lo = shift(lo, **{second: 1})
    right_lo = shift(lo, **{second: -1})
    left_hi = shift(hi, **{second: 1})
    right_hi = shift(hi, **{second: -1})
    far_lo = shift(left_lo, **{second: 1})
    far_hi = shift(right_hi, **{second: -1})
    return [lo, hi, left_lo, left_hi, right_lo, right_hi, far_lo, far_hi]


def spread_rows(pieces, first):
    return [pieces[0]] + [shift(p, **{first: r}) for p, r in zip(pieces[1:], REL[1:])]


def reduce_direct(parts, first, second):
    arrived = [parts[0]] + [shift(p, **{second: r}) for p, r in zip(parts[1:], REL[1:])]
    rows = parts[0].shape[0] // 4
    pieces = call(stage_kernel, tuple(shape(rows, D) for _ in REL))(*arrived)
    return spread_rows(pieces, first)


def reduce_ring(parts, first, second):
    own_lo, own_hi, left_lo, left_hi, right_lo, right_hi, far_lo, far_hi = parts
    n = far_lo.shape[0]
    from_right = shift(far_lo, **{second: -1})
    from_left = shift(far_hi, **{second: 1})
    r_hi = shift(left_hi, **{second: -1})
    l_lo = shift(right_lo, **{second: 1})
    left_lo, right_hi = call(relay_kernel, (shape(n, D), shape(n, D)))(
        left_lo, right_hi, from_right, from_left
    )
    r_lo = shift(left_lo, **{second: -1})
    l_hi = shift(right_hi, **{second: 1})
    pieces = call(halves_kernel, tuple(shape(n // 2, D) for _ in REL))(
        own_lo, own_hi, r_lo, r_hi, l_lo, l_hi
    )
    return spread_rows(pieces, first)


def body(tokens, gate_codes, gate_scales, up_codes, up_scales, cotangent):
    sources = (gate_codes, gate_scales.T, up_codes, up_scales.T)
    cube_shape = jax.ShapeDtypeStruct((NZ, TOK, SLICE), BF16)
    hbm = pl.BlockSpec(memory_space=pltpu.HBM)
    inputs = sources + (tokens, cotangent)
    shard_a, shard_b, copies, cot_sent = call(
        dequant_kernel,
        (shape(SHARD_A, D), shape(SHARD_B, D), cube_shape, shape(TOK, NY * HALF)),
        8,
        in_specs=[hbm] * 6,
        out_specs=(VMEM, VMEM, hbm, VMEM),
        scratch_shapes=[pltpu.VMEM(v.shape, v.dtype) for v in inputs]
        + [pltpu.SemaphoreType.DMA((len(inputs) + NZ,))],
    )(in_hbm(tokens), in_hbm(cotangent), *[in_hbm(v) for v in sources])
    wa = gather_plane(shard_a, "dx", "dy")
    wb = gather_plane(shard_b, "dy", "dx")

    mine = exchange_z(copies)
    theirs = shift(mine, dc=1)
    whole = call(join_kernel, shape(2 * TOK, D), 8)(mine, theirs)

    cot = call(spread_kernel, shape(2 * TOK, WIDE))(cotangent, shift(cot_sent, dz=4))

    def forward(w, half, lower, *before):
        shard = 2 * half
        width = 16 * shard
        total = lower + width
        return call(
            functools.partial(forward_kernel, shard, half, lower),
            (shape(TOK, total), shape(TOK, total), shape(2 * TOK, width)),
            scratch_shapes=[pltpu.VMEM((2 * TOK, width), F32)],
        )(whole, cot, *w, *before)

    def weight_grad(dd, count):
        outs = (shape(dd.shape[1] // count, D),) * count
        return call(weight_grad_kernel, outs)(dd, whole)

    hm_a, hp_a, dd_a = forward(wa, HALF_A, 0)
    hidden_mine, hidden_sent, dd_b = forward(wb, HALF_B, WIDE_A, hm_a, hp_a)
    sums_a = reduce_ring(weight_grad(dd_a, 8), "dx", "dy")
    sums_b = reduce_direct(weight_grad(dd_b, 4), "dy", "dx")

    quad = jax.ShapeDtypeStruct((2, NZL, TOK, SLICE), BF16)
    own_tg, other_tg = call(token_grad_kernel, (quad, quad), 20)(
        dd_a, dd_b, *wa, *wb
    )
    cube = (NZ, TOK, SLICE)
    received = shift(other_tg, dc=1)
    blocks = call(pair_sum_kernel, cube_shape, 8)(own_tg.reshape(cube), received.reshape(cube))
    gate_grad, up_grad, token_grad = call(
        finish_kernel, (shape(ROWS, D, F32), shape(ROWS, D, F32), shape(TOK, SLICE))
    )(*sums_a, *sums_b, exchange_z(blocks))

    hidden = call(
        collect_kernel,
        shape(TOK, GROUPS * ROWS),
        grid=(2,),
        in_specs=[whole_block(TOK, WIDE), whole_block(TOK, WIDE)],
        out_specs=whole_block(TOK, GROUPS * ROWS),
        scratch_shapes=[pltpu.VMEM((TOK, GROUPS * ROWS), F32)],
    )(hidden_mine, shift(hidden_sent, dz=4))
    return hidden, token_grad, gate_grad, up_grad


def solution(mesh):
    fine = Mesh(mesh.devices.reshape(NY, NZH, NX, NZL, NC), AXES)
    inter, intra = ("y", "zh", "x"), ("zl", "core")
    rows, toks = P(intra + inter, None), P(inter, intra)
    return jax.shard_map(
        body,
        mesh=fine,
        in_specs=(toks, rows, rows, rows, rows, toks),
        out_specs=(toks, toks, rows, rows),
        check_vma=False,
    )
```
